8 devices in a mesh: dp: 2 (over z, y), ep: 4 (over x, core).
Axes of the slice: x: 2, y: 2, z: 1, core: 2. Of those that a mesh axis runs over, the one named last changes fastest.
Arguments:
- hidden: bfloat16 [8192, 2048], P(('dp', 'ep')), parts along dimension 0
- expert_ids: int32 [8192, 2], P(('dp', 'ep')), parts along dimension 0
- norm_gain: bfloat16 [2048], replicated
- w_router: bfloat16 [2048, 8], replicated
- w_gate: bfloat16 [8, 2048, 5632], P('ep')
- w_up: bfloat16 [8, 2048, 5632], P('ep')
- w_down: bfloat16 [8, 5632, 2048], P('ep')
Outputs:
- output: bfloat16 [8192, 2048], P(('dp', 'ep')), parts along dimension 0
There are 2 independent parts. The reference program is written for one: setup_inputs(seed, part) draws one part's arguments, and reference() takes and returns one part's arrays. A program takes and returns all parts, laid end to end along the dimension named above; an argument that names none is the same for every part.
All inputs are finite; a program needn't handle non-finite values.
Results may differ from the reference program's by a relative error of at most 0.00119.
Values are sent between devices in bfloat16 or wider.
A program may use at most 1 GiB of HBM per device.

```python
import jax
import jax.numpy as jnp
from jax import lax

D = 2048
FF = 5632
EXPERTS = 8
TOK = 1024
GROUP = 4
NORM_EPS = 1e-5
TOKENS = TOK * GROUP
CAPACITY = (5 * TOK + 2 * EXPERTS - 1) // (2 * EXPERTS)


def draw_expert_ids(key):
    k_hot, k_ticket, k_cover, k_offset = jax.random.split(key, 4)
    hot_expert = jax.random.randint(k_hot, (GROUP, 1), 0, EXPERTS)
    ticket = jax.random.randint(k_ticket, (GROUP, TOK), 0, EXPERTS + 3)
    first_pick = jnp.where(ticket < EXPERTS, ticket, hot_expert)
    token_pos = jnp.arange(TOK)[None, :]
    cover_shift = jax.random.randint(k_cover, (GROUP, 1), 0, EXPERTS)
    first_pick = jnp.where(token_pos < EXPERTS, (token_pos + cover_shift) % EXPERTS, first_pick)
    offset = jax.random.randint(k_offset, (GROUP, TOK), 1, EXPERTS)
    second_pick = (first_pick + offset) % EXPERTS
    return jnp.stack([first_pick, second_pick], axis=-1).reshape(TOKENS, 2).astype(jnp.int32)


def setup_inputs(seed: int = 0, part: int = 0) -> dict:
    key = jax.random.key(seed)
    k_hidden, k_ids, k_gain, k_router, k_gate, k_up, k_down = jax.random.split(key, 7)
    k_hidden = jax.random.fold_in(k_hidden, part)
    k_ids = jax.random.fold_in(k_ids, part)
    hidden = jax.random.normal(k_hidden, (TOKENS, D), jnp.float32).astype(jnp.bfloat16)
    expert_ids = draw_expert_ids(k_ids)
    norm_gain = (1.0 + 0.3 * jax.random.normal(k_gain, (D,), jnp.float32)).astype(jnp.bfloat16)
    w_router = (2.0 * D ** -0.5 * jax.random.normal(k_router, (D, EXPERTS), jnp.float32)).astype(jnp.bfloat16)
    w_gate = (D ** -0.5 * jax.random.normal(k_gate, (EXPERTS, D, FF), jnp.float32)).astype(jnp.bfloat16)
    w_up = (D ** -0.5 * jax.random.normal(k_up, (EXPERTS, D, FF), jnp.float32)).astype(jnp.bfloat16)
    w_down = (2.0 * FF ** -0.5 * jax.random.normal(k_down, (EXPERTS, FF, D), jnp.float32)).astype(jnp.bfloat16)
    return {"hidden": hidden, "expert_ids": expert_ids, "norm_gain": norm_gain, "w_router": w_router, "w_gate": w_gate, "w_up": w_up, "w_down": w_down}


def rms_norm(hidden, norm_gain):
    hidden_f32 = hidden.astype(jnp.float32)
    mean_sq = jnp.mean(hidden_f32 * hidden_f32, axis=-1, keepdims=True)
    return (hidden_f32 * lax.rsqrt(mean_sq + NORM_EPS) * norm_gain.astype(jnp.float32)).astype(jnp.bfloat16)


def slot_positions(shard_ids):
    slot_order = jnp.concatenate([shard_ids[:, 0], shard_ids[:, 1]])
    hit_table = (slot_order[:, None] == jnp.arange(EXPERTS)[None, :]).astype(jnp.int32)
    seen_before = jnp.cumsum(hit_table, axis=0) - hit_table
    slot_rank = jnp.sum(seen_before * hit_table, axis=1)
    return slot_rank.reshape(2, TOK).T


def expert_ffn(operands):
    rows, gate_w, up_w, down_w = operands
    gate_proj = jnp.dot(rows, gate_w, preferred_element_type=jnp.float32)
    up_proj = jnp.dot(rows, up_w, preferred_element_type=jnp.float32)
    hidden_act = (jax.nn.silu(gate_proj) * up_proj).astype(jnp.bfloat16)
    return jnp.dot(hidden_act, down_w, preferred_element_type=jnp.float32).astype(jnp.bfloat16)


def reference(hidden, expert_ids, norm_gain, w_router, w_gate, w_up, w_down):
    normed = rms_norm(hidden, norm_gain)
    logits = jnp.dot(normed, w_router, preferred_element_type=jnp.float32)
    picked = jnp.take_along_axis(logits, expert_ids, axis=1)
    gate_probs = jax.nn.softmax(picked, axis=-1)
    positions = jax.vmap(slot_positions)(expert_ids.reshape(GROUP, TOK, 2)).reshape(TOKENS, 2)
    source = (jnp.arange(TOKENS) // TOK)[:, None]
    kept = positions < CAPACITY
    buffer_row = jnp.where(kept, source * CAPACITY + positions, GROUP * CAPACITY)
    rows_in = jnp.broadcast_to(normed[:, None, :], (TOKENS, 2, D))
    buffers = jnp.zeros((EXPERTS, GROUP * CAPACITY, D), jnp.bfloat16)
    buffers = buffers.at[expert_ids, buffer_row].set(rows_in, mode="drop")
    expert_out = lax.map(expert_ffn, (buffers, w_gate, w_up, w_down))
    fetched = expert_out[expert_ids, jnp.minimum(buffer_row, GROUP * CAPACITY - 1)]
    fetched = jnp.where(kept[:, :, None], fetched.astype(jnp.float32), 0.0)
    mixed_sum = jnp.sum(gate_probs[:, :, None] * fetched, axis=1)
    return (hidden.astype(jnp.float32) + mixed_sum).astype(jnp.bfloat16)
```

```python
import functools

import jax
import jax.numpy as jnp
from jax import lax
from jax.experimental import pallas as pl
from jax.experimental.pallas import tpu as pltpu
from jax.sharding import PartitionSpec as P


NORM_EPS = 1e-5
F32 = jnp.float32
BF16 = jnp.bfloat16
BLK = 16
NBUF = 3
TF = 512
ANY = pl.BlockSpec(memory_space=pl.ANY)
SMEM = pl.BlockSpec(memory_space=pltpu.SMEM)
VMEM = pl.BlockSpec(memory_space=pltpu.VMEM)
MIB = 2**20


def up_to(n, m):
    return (n + m - 1) // m * m


def pack_rows(normed, queue, expert, cap):
    place = queue[pl.ds(expert, 1), :]
    rows = lax.broadcasted_iota(jnp.int32, (cap, place.shape[1]), 0)
    pick = (rows == place).astype(F32).astype(BF16)
    return jnp.dot(pick, normed, preferred_element_type=F32).astype(BF16)


def route_kernel(cap, exps, hid, ids, idst, gain, w_router, normed, queue, codes, gates, counts, *far0):
    tok, _ = hid.shape
    experts = w_router.shape[1]
    step = 256
    for i in range(0, tok, step):
        x = hid[i:i + step, :].astype(F32)
        mean_sq = jnp.mean(x * x, axis=-1, keepdims=True)
        normed[i:i + step, :] = (x * lax.rsqrt(mean_sq + NORM_EPS) * gain[...].astype(F32)).astype(BF16)

    eye_t = lax.broadcasted_iota(jnp.int32, (experts, tok), 0)
    hit0_t = (idst[0:1, :] == eye_t).astype(F32)
    hit1_t = (idst[1:2, :] == eye_t).astype(F32)
    tot0_t = jnp.sum(hit0_t, axis=1, keepdims=True)
    tot1_t = jnp.sum(hit1_t, axis=1, keepdims=True)
    both_t = jnp.concatenate([hit0_t, hit1_t], axis=0).astype(BF16)
    for i in range(0, tok, step):
        before = (lax.broadcasted_iota(jnp.int32, (tok, step), 0)
                  < i + lax.broadcasted_iota(jnp.int32, (tok, step), 1)).astype(F32).astype(BF16)
        seen = jnp.dot(both_t, before, preferred_element_type=F32)
        h0, h1 = hit0_t[:, i:i + step], hit1_t[:, i:i + step]
        place = jnp.where(h0 > 0, seen[:experts], jnp.where(h1 > 0, seen[experts:] + tot0_t, -1.0))
        queue[:, i:i + step] = place.astype(jnp.int32)
    counts[...] = jnp.broadcast_to(jnp.minimum(tot0_t + tot1_t, float(cap)), counts.shape).astype(jnp.int32)

    eye = lax.broadcasted_iota(jnp.int32, (tok, experts), 1)
    hit0 = (ids[:, 0:1] == eye).astype(F32)
    hit1 = (ids[:, 1:2] == eye).astype(F32)
    tot0 = jnp.sum(hit0, axis=0, keepdims=True)
    both = jnp.concatenate([hit0, hit1], axis=1).astype(BF16)
    for i in range(0, tok, step):
        before = (i + lax.broadcasted_iota(jnp.int32, (step, tok), 0)
                  > lax.broadcasted_iota(jnp.int32, (step, tok), 1)).astype(F32).astype(BF16)
        seen = jnp.dot(before, both, preferred_element_type=F32)
        h0, h1 = hit0[i:i + step], hit1[i:i + step]
        logits = jnp.dot(normed[i:i + step, :], w_router[...], preferred_element_type=F32)
        pos0 = jnp.sum(h0 * seen[:, :experts], axis=1, keepdims=True).astype(jnp.int32)
        pos1 = jnp.sum(h1 * (seen[:, experts:] + tot0), axis=1, keepdims=True).astype(jnp.int32)
        code0 = jnp.where(pos0 < cap, ids[i:i + step, 0:1] * cap + pos0, -1)
        code1 = jnp.where(pos1 < cap, ids[i:i + step, 1:2] * cap + pos1, -1)
        l0 = jnp.sum(h0 * logits, axis=1, keepdims=True)
        l1 = jnp.sum(h1 * logits, axis=1, keepdims=True)
        top = jnp.maximum(l0, l1)
        e0, e1 = jnp.exp(l0 - top), jnp.exp(l1 - top)
        codes[i:i + step, 0:1] = code0
        codes[i:i + step, 1:2] = code1
        gates[i:i + step, 0:1] = e0 / (e0 + e1)
        gates[i:i + step, 1:2] = e1 / (e0 + e1)

    for k in range(2):
        far0[k][...] = pack_rows(normed[...], queue, exps[k], cap)


def route(exps, hidden, ids, gain, w_router, cap):
    tok, width = hidden.shape
    experts = w_router.shape[1]
    one = jax.ShapeDtypeStruct((cap, width), BF16)
    return pl.pallas_call(
        functools.partial(route_kernel, cap),
        out_shape=[jax.ShapeDtypeStruct((tok, width), BF16), jax.ShapeDtypeStruct((experts, tok), jnp.int32),
                   jax.ShapeDtypeStruct((tok, 2), jnp.int32), jax.ShapeDtypeStruct((tok, 2), F32),
                   jax.ShapeDtypeStruct((experts, 128), jnp.int32), one, one],
        in_specs=[SMEM] + [VMEM] * 5,
        out_specs=[VMEM] * 7,
        cost_estimate=pl.CostEstimate(flops=10**10, bytes_accessed=2 * 10**7, transcendentals=0),
        compiler_params=pltpu.CompilerParams(vmem_limit_bytes=48 * MIB),
    )(exps, hidden, ids, ids.T, gain.reshape(1, width), w_router)


def pack_kernel(cap, exps, normed, queue, *outs):
    for k, out in enumerate(outs):
        out[...] = pack_rows(normed[...], queue, exps[k], cap)


def pack(exps, normed, queue, cap):
    _, width = normed.shape
    one = jax.ShapeDtypeStruct((cap, width), BF16)
    return pl.pallas_call(
        functools.partial(pack_kernel, cap),
        out_shape=[one] * exps.shape[0],
        in_specs=[SMEM] + [VMEM] * 2,
        out_specs=[VMEM] * exps.shape[0],
        cost_estimate=pl.CostEstimate(flops=9 * 10**9, bytes_accessed=2 * 10**7, transcendentals=0),
        compiler_params=pltpu.CompilerParams(vmem_limit_bytes=48 * MIB),
    )(exps, normed, queue)


def ffn_kernel(local, cap, sizes, counts, x0, x1, wg, wu, wd, o0, o1, xs, acc, bg, bu, bd, wsem, sem):
    steps = wg.shape[2] // TF
    n0 = pl.multiple_of((counts[0] + BLK - 1) // BLK * BLK, BLK)
    rows = n0 + counts[1]

    def copies(f, slot):
        cols = pl.ds(pl.multiple_of(f * TF, TF), TF)
        return (pltpu.make_async_copy(wg.at[local, :, cols], bg.at[slot], wsem.at[0, slot]),
                pltpu.make_async_copy(wu.at[local, :, cols], bu.at[slot], wsem.at[1, slot]),
                pltpu.make_async_copy(wd.at[local, cols, :], bd.at[slot], wsem.at[2, slot]))

    def fetch(f, slot):
        for c in copies(f, slot):
            c.start()

    first = pltpu.make_async_copy(x0, xs.at[pl.ds(0, cap)], sem.at[0])
    first.start()
    for s in range(NBUF - 1):
        fetch(s, s)
    acc[...] = jnp.zeros_like(acc)
    first.wait()
    second = pltpu.make_async_copy(x1, xs.at[pl.ds(n0, cap)], sem.at[1])
    second.start()
    second.wait()

    def step(f, _):
        slot = lax.rem(f, NBUF)
        for c in copies(f, slot):
            c.wait()

        @pl.when(f + NBUF - 1 < steps)
        def _():
            fetch(f + NBUF - 1, lax.rem(f + NBUF - 1, NBUF))

        def tile(m):
            x = xs[0:m, :]
            g = jnp.dot(x, bg[slot], preferred_element_type=F32)
            u = jnp.dot(x, bu[slot], preferred_element_type=F32)
            a = (jax.nn.silu(g) * u).astype(BF16)
            acc[0:m, :] += jnp.dot(a, bd[slot], preferred_element_type=F32)

        low = 0
        for m in sizes:
            @pl.when((rows > low) & (rows <= m))
            def _():
                tile(m)

            low = m
        return 0

    lax.fori_loop(0, steps, step, 0)
    xs[...] = acc[...].astype(BF16)
    a = pltpu.make_async_copy(xs.at[pl.ds(0, cap)], o0, sem.at[0])
    b = pltpu.make_async_copy(xs.at[pl.ds(n0, cap)], o1, sem.at[1])
    a.start()
    b.start()
    a.wait()
    b.wait()


def ffn(counts, xs, wg, wu, wd, local, cap):
    width, inner = wg.shape[1:]
    sizes = (2 * cap - 256, 2 * cap - 192, 2 * cap - 128, 2 * cap - 64, 2 * cap)
    return pl.pallas_call(
        functools.partial(ffn_kernel, local, cap, sizes),
        out_shape=[jax.ShapeDtypeStruct(x.shape, BF16) for x in xs],
        in_specs=[SMEM] + [ANY] * (3 + len(xs)),
        out_specs=[ANY] * len(xs),
        scratch_shapes=[pltpu.VMEM((2 * cap, width), BF16), pltpu.VMEM((2 * cap, width), F32),
                        pltpu.VMEM((NBUF, width, TF), BF16), pltpu.VMEM((NBUF, width, TF), BF16),
                        pltpu.VMEM((NBUF, TF, width), BF16),
                        pltpu.SemaphoreType.DMA((3, NBUF)), pltpu.SemaphoreType.DMA((2,))],
        cost_estimate=pl.CostEstimate(flops=6 * 540 * width * inner, bytes_accessed=6 * width * inner, transcendentals=0),
        compiler_params=pltpu.CompilerParams(vmem_limit_bytes=60 * MIB),
    )(counts, *xs, wg, wu, wd)


def merge_kernel(cap, n_buf, final, counts, tgt, codes, gates, base, *refs):
    bufs, out, held = refs[:n_buf], refs[n_buf], refs[n_buf + 1]

    @pl.when(pl.program_id(0) == 0)
    def _():
        at, seg = 0, 0
        for buf in bufs:
            for i in range(0, buf.shape[0], cap):
                live = lax.broadcasted_iota(jnp.int32, (cap, buf.shape[1]), 0) < counts[seg]
                part = buf[i:i + cap, :].astype(F32)
                held[at:at + cap, :] = jnp.where(live, part, 0.0).astype(BF16)
                at, seg = at + cap, seg + 1
        if at < held.shape[0]:
            held[at:, :] = jnp.zeros((held.shape[0] - at, held.shape[1]), BF16)

    got = []
    for s in range(2):
        pick = (codes[:, s:s + 1] == tgt[...]).astype(F32).astype(BF16)
        got.append(gates[:, s:s + 1] * jnp.dot(pick, held[...], preferred_element_type=F32))
    total = got[0] + got[1]
    if base is not None:
        total = base[0][...] + total
    if final:
        total = base[1][...].astype(F32) + total
    out[...] = total.astype(out.dtype)


def merge(experts_of, counts, codes, gates, bufs, cap, partial=None, hidden=None):
    tok, width = codes.shape[0], bufs[0].shape[1]
    deep = up_to(len(experts_of) * cap, 256)
    tgt = (jnp.stack(experts_of)[:, None] * cap + jnp.arange(cap)[None, :]).reshape(1, -1)
    tgt = jnp.pad(tgt, ((0, 0), (0, deep - tgt.shape[1])), constant_values=-2).astype(jnp.int32)
    final = hidden is not None
    rows = 256
    tile = pl.BlockSpec((rows, width), lambda i: (i, 0))
    pair = pl.BlockSpec((rows, 2), lambda i: (i, 0))
    extra = [partial, hidden] if final else []
    n_buf = len(bufs)

    def body(counts, tgt, codes, gates, *refs):
        base = refs[:len(extra)] if extra else None
        merge_kernel(cap, n_buf, final, counts, tgt, codes, gates, base, *refs[len(extra):])

    return pl.pallas_call(
        body,
        out_shape=jax.ShapeDtypeStruct((tok, width), BF16 if final else F32),
        grid=(tok // rows,),
        in_specs=[SMEM, pl.BlockSpec((1, deep), lambda i: (0, 0)), pair, pair] + [tile] * len(extra)
        + [pl.BlockSpec(b.shape, lambda i: (0, 0)) for b in bufs],
        out_specs=tile,
        scratch_shapes=[pltpu.VMEM((deep, width), BF16)],
        cost_estimate=pl.CostEstimate(flops=4 * tok * deep * width, bytes_accessed=2 * 10**7, transcendentals=0),
        compiler_params=pltpu.CompilerParams(vmem_limit_bytes=56 * MIB),
    )(jnp.stack(counts), tgt, codes, gates, *extra, *bufs)


def solution(mesh):
    token_spec = P(("dp", "ep"), None)
    expert_spec = P("ep", None, None)

    def local_block(hidden, expert_ids, norm_gain, w_router, w_gate, w_up, w_down):
        tok, _ = hidden.shape
        experts = w_router.shape[1]
        per = w_gate.shape[0]
        group = experts // per
        cap = (5 * tok + 2 * experts - 1) // (2 * experts)
        me = lax.axis_index("ep")
        peer = [me ^ k for k in range(group)]

        def swap(x, k):
            return lax.ppermute(x, "ep", [(i, i ^ k) for i in range(group)])

        def ids_of(pairs):
            return [per * peer[k] + i for k, i in pairs]

        def after(x, *earlier):
            return lax.optimization_barrier((x, *earlier))[0]

        normed, queue, codes, gates, n_mine, *far0 = route(
            jnp.stack(ids_of([(2, 0), (3, 0)])), hidden, expert_ids, norm_gain, w_router, cap)
        got0 = [swap(far0[0], 2), swap(far0[1], 3)]
        n_all = lax.all_gather(n_mine[:, 0], "ep")
        own0, sib0, own1, sib1, *far1 = pack(
            jnp.stack(ids_of([(0, 0), (1, 0), (0, 1), (1, 1), (2, 1), (3, 1)])), normed, queue, cap)
        sib0, sib1 = swap(sib0, 1), swap(sib1, 1)
        got1 = [swap(far1[0], 2), swap(far1[1], 3)]

        def run(i, k, xs, *earlier):
            expert = per * me + i
            counts = jnp.stack([n_all[peer[k], expert], n_all[peer[k + 1], expert]])
            return ffn(after(counts, *earlier), xs, w_gate, w_up, w_down, i, cap)

        o_own0, o_sib0 = run(0, 0, [own0, sib0])
        o_far0 = run(0, 2, got0, o_own0)
        back0 = [swap(o_far0[0], 2), swap(o_far0[1], 3)]
        o_far1 = run(1, 2, got1, o_far0[0])
        back1 = [swap(o_far1[0], 2), swap(o_far1[1], 3)]
        o_own1, o_sib1 = run(1, 0, [own1, sib1], o_far1[0])
        back_sib = [swap(o_sib0, 1), swap(o_sib1, 1)]

        def gather(pairs, bufs, **kw):
            experts_of = ids_of(pairs)
            return merge(experts_of, [n_all[me, e] for e in experts_of], codes, gates, bufs, cap, **kw)

        partial = gather([(0, 0), (1, 0), (0, 1), (1, 1), (2, 0), (3, 0)],
                         [o_own0, back_sib[0], o_own1, back_sib[1]] + back0)
        return gather([(2, 1), (3, 1)], back1, partial=partial, hidden=hidden)

    return jax.shard_map(local_block, mesh=mesh,
                         in_specs=(token_spec, token_spec, P(None), P(None, None), expert_spec, expert_spec, expert_spec),
                         out_specs=token_spec, check_vma=False)
```

```python
import functools

import jax
import jax.numpy as jnp
from jax import lax
from jax.experimental import pallas as pl
from jax.experimental.pallas import tpu as pltpu
from jax.sharding import PartitionSpec as P


NORM_EPS = 1e-5
F32 = jnp.float32
BF16 = jnp.bfloat16
BLK = 16
NBUF = 3
TF = 512
ANY = pl.BlockSpec(memory_space=pl.ANY)
SMEM = pl.BlockSpec(memory_space=pltpu.SMEM)
VMEM = pl.BlockSpec(memory_space=pltpu.VMEM)
HBM = pl.BlockSpec(memory_space=pltpu.HBM)
MIB = 2**20


def up_to(n, m):
    return (n + m - 1) // m * m


def peers_of(group):
    me = lax.axis_index("ep")
    return [me, me + 1 - 2 * lax.rem(me, 2), lax.rem(me + 2, group), group - 1 - me]


def tally_kernel(group, cap, idst, table, mine, held, send_sem, recv_sem):
    experts = held.shape[1]
    peers = peers_of(group)
    eye = lax.broadcasted_iota(jnp.int32, (experts, idst.shape[1]), 0)
    hits = ((idst[0:1, :] == eye) | (idst[1:2, :] == eye)).astype(F32).astype(BF16)
    ones = jnp.ones((8, idst.shape[1]), BF16)
    total = lax.dot_general(ones, hits, (((1,), (1,)), ((), ())), preferred_element_type=F32)
    mine[...] = jnp.zeros_like(mine)
    mine[:, 0:experts] = jnp.minimum(total, float(cap)).astype(jnp.int32)
    barrier = pltpu.get_barrier_semaphore()
    for peer in peers[1:]:
        pl.semaphore_signal(barrier, inc=1, device_id={"ep": peer}, device_id_type=pl.DeviceIdType.MESH)
    pl.semaphore_wait(barrier, group - 1)
    sends = [pltpu.make_async_remote_copy(
        src_ref=mine, dst_ref=held.at[k], send_sem=send_sem.at[k], recv_sem=recv_sem.at[k],
        device_id={"ep": peers[k]}, device_id_type=pl.DeviceIdType.MESH) for k in range(1, group)]
    for copy in sends:
        copy.start()
    table[...] = jnp.zeros_like(table)
    table[0:1, :] = mine[0:1, :]
    for k, copy in enumerate(sends):
        copy.wait()
        table[k + 1:k + 2, :] = held[k + 1, 0:1, :]


def tally(idst, experts, group, cap):
    return pl.pallas_call(
        functools.partial(tally_kernel, group, cap),
        out_shape=jax.ShapeDtypeStruct((8, 128), jnp.int32),
        in_specs=[VMEM], out_specs=VMEM,
        scratch_shapes=[pltpu.VMEM((8, 128), jnp.int32), pltpu.VMEM((group, experts, 128), jnp.int32),
                        pltpu.SemaphoreType.DMA((group,)), pltpu.SemaphoreType.DMA((group,))],
        compiler_params=pltpu.CompilerParams(collective_id=0, has_side_effects=True),
    )(idst)


def pack_rows(normed, queue, expert, cap):
    place = queue[pl.ds(expert, 1), :]
    rows = lax.broadcasted_iota(jnp.int32, (cap, place.shape[1]), 0)
    pick = (rows == place).astype(F32).astype(BF16)
    return jnp.dot(pick, normed, preferred_element_type=F32).astype(BF16)


def emit_packs(cap, normed, queue, experts_of, outs, slots, sem):
    copies = []
    for k, (expert, out) in enumerate(zip(experts_of, outs)):
        slots[k] = pack_rows(normed[...], queue, expert, cap)
        copies.append(pltpu.make_async_copy(slots.at[k], out, sem.at[k]))
        copies[-1].start()
    for copy in copies:
        copy.wait()


def route_kernel(group, per, cap, hid, idst, gain, w_router_t, normed, queue, meta, *rest):
    far0, (slots, sem) = rest[:2], rest[2:]
    tok = hid.shape[0]
    experts = w_router_t.shape[0]
    step = 256
    for i in range(0, tok, step):
        x = hid[i:i + step, :].astype(F32)
        mean_sq = jnp.mean(x * x, axis=-1, keepdims=True)
        normed[i:i + step, :] = (x * lax.rsqrt(mean_sq + NORM_EPS) * gain[...].astype(F32)).astype(BF16)
    logits = lax.dot_general(w_router_t[...], normed[...], (((1,), (1,)), ((), ())), preferred_element_type=F32)

    eye = lax.broadcasted_iota(jnp.int32, (experts, tok), 0)
    hit0 = (idst[0:1, :] == eye).astype(F32)
    hit1 = (idst[1:2, :] == eye).astype(F32)
    tot0 = jnp.sum(hit0, axis=1, keepdims=True)
    both = jnp.concatenate([hit0, hit1], axis=0).astype(BF16)
    parts = []
    for i in range(0, tok, step):
        before = (lax.broadcasted_iota(jnp.int32, (tok, step), 0)
                  < i + lax.broadcasted_iota(jnp.int32, (tok, step), 1)).astype(F32).astype(BF16)
        parts.append(jnp.dot(both, before, preferred_element_type=F32))
    seen = jnp.concatenate(parts, axis=1)
    place = jnp.where(hit0 > 0, seen[:experts], jnp.where(hit1 > 0, seen[experts:] + tot0, -1.0))
    queue[...] = place.astype(jnp.int32)

    base = eye.astype(F32) * float(cap)
    kept = place < float(cap)
    code = jnp.where(kept, base + place, -1.0)
    l0 = jnp.sum(hit0 * logits, axis=0, keepdims=True)
    l1 = jnp.sum(hit1 * logits, axis=0, keepdims=True)
    top = jnp.maximum(l0, l1)
    e0, e1 = jnp.exp(l0 - top), jnp.exp(l1 - top)
    lines = jnp.concatenate([jnp.sum(hit0 * code, axis=0, keepdims=True), jnp.sum(hit1 * code, axis=0, keepdims=True),
                             e0 / (e0 + e1), e1 / (e0 + e1), jnp.zeros((4, tok), F32)], axis=0)
    meta[...] = lines.T
    peers = peers_of(group)
    emit_packs(cap, normed, queue, [per * peers[2], per * peers[3]], far0, slots, sem)


def route(hidden, idst, gain, w_router_t, group, cap):
    tok, width = hidden.shape
    experts = w_router_t.shape[0]
    one = jax.ShapeDtypeStruct((cap, width), BF16)
    return pl.pallas_call(
        functools.partial(route_kernel, group, experts // group, cap),
        out_shape=[jax.ShapeDtypeStruct((tok, width), BF16), jax.ShapeDtypeStruct((experts, tok), jnp.int32),
                   jax.ShapeDtypeStruct((tok, 8), F32), one, one],
        in_specs=[VMEM] * 4,
        out_specs=[VMEM] * 3 + [HBM] * 2,
        scratch_shapes=[pltpu.VMEM((2, cap, width), BF16), pltpu.SemaphoreType.DMA((2,))],
        cost_estimate=pl.CostEstimate(flops=10**10, bytes_accessed=2 * 10**7, transcendentals=0),
        compiler_params=pltpu.CompilerParams(vmem_limit_bytes=48 * MIB),
    )(hidden, idst, gain, w_router_t)


def pack_kernel(group, per, cap, pairs, normed, queue, *rest):
    outs, (slots, sem) = rest[:len(pairs)], rest[len(pairs):]
    peers = peers_of(group)
    emit_packs(cap, normed, queue, [per * peers[k] + i for k, i in pairs], outs, slots, sem)


def pack(pairs, normed, queue, group, cap):
    _, width = normed.shape
    n = len(pairs)
    return pl.pallas_call(
        functools.partial(pack_kernel, group, queue.shape[0] // group, cap, pairs),
        out_shape=[jax.ShapeDtypeStruct((cap, width), BF16)] * n,
        in_specs=[VMEM] * 2,
        out_specs=[HBM] * n,
        scratch_shapes=[pltpu.VMEM((n, cap, width), BF16), pltpu.SemaphoreType.DMA((n,))],
        cost_estimate=pl.CostEstimate(flops=9 * 10**9, bytes_accessed=2 * 10**7, transcendentals=0),
        compiler_params=pltpu.CompilerParams(vmem_limit_bytes=48 * MIB),
    )(normed, queue)


def ffn_kernel(local, per, dist, cap, sizes, table, x0, x1, wg, wu, wd, o0, o1, xs, acc, bg, bu, bd, wsem, sem):
    steps = wg.shape[2] // TF
    expert = per * lax.axis_index("ep") + local
    n0 = pl.multiple_of((table[dist, expert] + BLK - 1) // BLK * BLK, BLK)
    rows = n0 + table[dist + 1, expert]

    def copies(f, slot):
        cols = pl.ds(pl.multiple_of(f * TF, TF), TF)
        return (pltpu.make_async_copy(wg.at[local, :, cols], bg.at[slot], wsem.at[0, slot]),
                pltpu.make_async_copy(wu.at[local, :, cols], bu.at[slot], wsem.at[1, slot]),
                pltpu.make_async_copy(wd.at[local, cols, :], bd.at[slot], wsem.at[2, slot]))

    def fetch(f, slot):
        for c in copies(f, slot):
            c.start()

    first = pltpu.make_async_copy(x0, xs.at[pl.ds(0, cap)], sem.at[0])
    first.start()
    for s in range(NBUF - 1):
        fetch(s, s)
    acc[...] = jnp.zeros_like(acc)
    first.wait()
    second = pltpu.make_async_copy(x1, xs.at[pl.ds(n0, cap)], sem.at[1])
    second.start()
    second.wait()

    def step(f, _):
        slot = lax.rem(f, NBUF)
        for c in copies(f, slot):
            c.wait()

        @pl.when(f + NBUF - 1 < steps)
        def _():
            fetch(f + NBUF - 1, lax.rem(f + NBUF - 1, NBUF))

        def tile(m):
            x = xs[0:m, :]
            g = jnp.dot(x, bg[slot], preferred_element_type=F32)
            u = jnp.dot(x, bu[slot], preferred_element_type=F32)
            a = (jax.nn.silu(g) * u).astype(BF16)
            acc[0:m, :] += jnp.dot(a, bd[slot], preferred_element_type=F32)

        low = 0
        for m in sizes:
            @pl.when((rows > low) & (rows <= m))
            def _():
                tile(m)

            low = m
        return 0

    lax.fori_loop(0, steps, step, 0)
    xs[...] = acc[...].astype(BF16)
    a = pltpu.make_async_copy(xs.at[pl.ds(0, cap)], o0, sem.at[0])
    b = pltpu.make_async_copy(xs.at[pl.ds(n0, cap)], o1, sem.at[1])
    a.start()
    b.start()
    a.wait()
    b.wait()


def ffn(table, xs, wg, wu, wd, local, dist, cap):
    width, inner = wg.shape[1:]
    sizes = (2 * cap - 256, 2 * cap - 192, 2 * cap - 128, 2 * cap - 64, 2 * cap)
    return pl.pallas_call(
        functools.partial(ffn_kernel, local, wg.shape[0], dist, cap, sizes),
        out_shape=[jax.ShapeDtypeStruct(x.shape, BF16) for x in xs],
        in_specs=[SMEM] + [ANY] * (3 + len(xs)),
        out_specs=[HBM] * len(xs),
        scratch_shapes=[pltpu.VMEM((2 * cap, width), BF16), pltpu.VMEM((2 * cap, width), F32),
                        pltpu.VMEM((NBUF, width, TF), BF16), pltpu.VMEM((NBUF, width, TF), BF16),
                        pltpu.VMEM((NBUF, TF, width), BF16),
                        pltpu.SemaphoreType.DMA((3, NBUF)), pltpu.SemaphoreType.DMA((2,))],
        cost_estimate=pl.CostEstimate(flops=6 * 540 * width * inner, bytes_accessed=6 * width * inner, transcendentals=0),
        compiler_params=pltpu.CompilerParams(vmem_limit_bytes=60 * MIB),
    )(table, *xs, wg, wu, wd)


def merge_kernel(group, per, cap, pairs, final, table, meta, *refs):
    extra, refs = refs[:2 * final], refs[2 * final:]
    bufs, (out, held, tgt) = refs[:len(pairs)], refs[len(pairs):]

    @pl.when(pl.program_id(0) == 0)
    def _():
        peers = peers_of(group)
        lane = lax.broadcasted_iota(jnp.int32, tgt.shape, 1)
        want = jnp.full(tgt.shape, -2, jnp.int32)
        for j, ((k, i), buf) in enumerate(zip(pairs, bufs)):
            expert = per * peers[k] + i
            want = jnp.where((lane >= j * cap) & (lane < (j + 1) * cap), expert * cap + lane - j * cap, want)
            live = lax.broadcasted_iota(jnp.int32, buf.shape, 0) < table[0, expert]
            held[j * cap:(j + 1) * cap, :] = jnp.where(live, buf[...].astype(F32), 0.0).astype(BF16)
        tgt[...] = want.astype(F32)
        at = len(pairs) * cap
        if at < held.shape[0]:
            held[at:, :] = jnp.zeros((held.shape[0] - at, held.shape[1]), BF16)

    total = None
    for s in range(2):
        pick = (meta[:, s:s + 1] == tgt[0:1, :]).astype(F32).astype(BF16)
        got = meta[:, s + 2:s + 3] * jnp.dot(pick, held[...], preferred_element_type=F32)
        total = got if total is None else total + got
    if final:
        total = extra[1][...].astype(F32) + (extra[0][...] + total)
    out[...] = total.astype(out.dtype)


def merge(pairs, table, meta, bufs, group, per, cap, partial=None, hidden=None):
    tok, width = meta.shape[0], bufs[0].shape[1]
    deep = up_to(len(pairs) * cap, 256)
    final = hidden is not None
    rows = 256
    tile = pl.BlockSpec((rows, width), lambda i: (i, 0))
    extra = [partial, hidden] if final else []
    return pl.pallas_call(
        functools.partial(merge_kernel, group, per, cap, pairs, final),
        out_shape=jax.ShapeDtypeStruct((tok, width), BF16 if final else F32),
        grid=(tok // rows,),
        in_specs=[SMEM, pl.BlockSpec((rows, 8), lambda i: (i, 0))] + [tile] * len(extra)
        + [pl.BlockSpec(b.shape, lambda i: (0, 0)) for b in bufs],
        out_specs=tile,
        scratch_shapes=[pltpu.VMEM((deep, width), BF16), pltpu.VMEM((8, deep), F32)],
        cost_estimate=pl.CostEstimate(flops=4 * tok * deep * width, bytes_accessed=2 * 10**7, transcendentals=0),
        compiler_params=pltpu.CompilerParams(vmem_limit_bytes=56 * MIB),
    )(table, meta, *extra, *bufs)


def solution(mesh):
    token_spec = P(("dp", "ep"), None)
    expert_spec = P("ep", None, None)

    def local_block(hidden, expert_ids, norm_gain, w_router, w_gate, w_up, w_down):
        tok, width = hidden.shape
        experts = w_router.shape[1]
        per = w_gate.shape[0]
        group = experts // per
        cap = (5 * tok + 2 * experts - 1) // (2 * experts)

        def swap(x, k):
            return lax.ppermute(x, "ep", [(i, i ^ k) for i in range(group)])

        def after(x, *earlier):
            return lax.optimization_barrier((x, *earlier))[0]

        idst = expert_ids.T
        table = tally(idst, experts, group, cap)
        normed, queue, meta, *far0 = route(
            hidden, after(idst, table), norm_gain.reshape(1, width), w_router.T, group, cap)
        got0 = [swap(far0[0], 2), swap(far0[1], 3)]
        own0, sib0, own1, sib1, *far1 = pack(
            [(0, 0), (1, 0), (0, 1), (1, 1), (2, 1), (3, 1)], normed, queue, group, cap)
        sib0, sib1 = swap(sib0, 1), swap(sib1, 1)
        got1 = [swap(far1[0], 2), swap(far1[1], 3)]

        def run(i, k, xs, *earlier):
            return ffn(after(table, *earlier), xs, w_gate, w_up, w_down, i, k, cap)

        o_own0, o_sib0 = run(0, 0, [own0, sib0])
        o_far0 = run(0, 2, got0, o_own0)
        back0 = [swap(o_far0[0], 2), swap(o_far0[1], 3)]
        o_far1 = run(1, 2, got1, o_far0[0])
        back1 = [swap(o_far1[0], 2), swap(o_far1[1], 3)]
        o_own1, o_sib1 = run(1, 0, [own1, sib1], o_far1[0])
        back_sib = [swap(o_sib0, 1), swap(o_sib1, 1)]

        def gather(pairs, bufs, **kw):
            return merge(pairs, table, meta, bufs, group, per, cap, **kw)

        partial = gather([(0, 0), (1, 0), (0, 1), (1, 1), (2, 0), (3, 0)],
                         [o_own0, back_sib[0], o_own1, back_sib[1]] + back0)
        return gather([(2, 1), (3, 1)], back1, partial=partial, hidden=hidden)

    return jax.shard_map(local_block, mesh=mesh,
                         in_specs=(token_spec, token_spec, P(None), P(None, None), expert_spec, expert_spec, expert_spec),
                         out_specs=token_spec, check_vma=False)
```

```python
import functools

import jax
import jax.numpy as jnp
from jax import lax
from jax.experimental import pallas as pl
from jax.experimental.pallas import tpu as pltpu
from jax.sharding import PartitionSpec as P


NORM_EPS = 1e-5
F32 = jnp.float32
BF16 = jnp.bfloat16
BLK = 16
NBUF = 3
TF = 512
ANY = pl.BlockSpec(memory_space=pl.ANY)
SMEM = pl.BlockSpec(memory_space=pltpu.SMEM)
VMEM = pl.BlockSpec(memory_space=pltpu.VMEM)
HBM = pl.BlockSpec(memory_space=pltpu.HBM)
MIB = 2**20


def up_to(n, m):
    return (n + m - 1) // m * m


def peers_of(group):
    me = lax.axis_index("ep")
    return [me, me + 1 - 2 * lax.rem(me, 2), lax.rem(me + 2, group), group - 1 - me]


def pack_rows(normed, queue, expert, cap):
    place = queue[pl.ds(expert, 1), :]
    rows = lax.broadcasted_iota(jnp.int32, (cap, place.shape[1]), 0)
    pick = (rows == place).astype(F32).astype(BF16)
    return jnp.dot(pick, normed, preferred_element_type=F32).astype(BF16)


def emit_packs(cap, normed, queue, experts_of, outs, slots, sem):
    copies = []
    for k, (expert, out) in enumerate(zip(experts_of, outs)):
        slots[k] = pack_rows(normed[...], queue, expert, cap)
        copies.append(pltpu.make_async_copy(slots.at[k], out, sem.at[k]))
        copies[-1].start()
    for copy in copies:
        copy.wait()


def route_kernel(group, per, cap, hid, idst, gain, w_router_t, normed, queue, meta, table, *rest):
    far0, (slots, sem, mine, held, send_sem, recv_sem) = rest[:2], rest[2:]
    peers = peers_of(group)
    barrier = pltpu.get_barrier_semaphore()
    for peer in peers[1:]:
        pl.semaphore_signal(barrier, inc=1, device_id={"ep": peer}, device_id_type=pl.DeviceIdType.MESH)

    tok = hid.shape[0]
    experts = w_router_t.shape[0]
    eye = lax.broadcasted_iota(jnp.int32, (experts, tok), 0)
    hit0 = (idst[0:1, :] == eye).astype(F32)
    hit1 = (idst[1:2, :] == eye).astype(F32)
    both = jnp.concatenate([hit0, hit1], axis=0).astype(BF16)
    total = lax.dot_general(jnp.ones((8, tok), BF16), (hit0 + hit1).astype(BF16), (((1,), (1,)), ((), ())),
                            preferred_element_type=F32)
    mine[...] = jnp.zeros_like(mine)
    mine[:, 0:experts] = jnp.minimum(total, float(cap)).astype(jnp.int32)

    step = 256
    for i in range(0, tok, step):
        x = hid[i:i + step, :].astype(F32)
        mean_sq = jnp.mean(x * x, axis=-1, keepdims=True)
        normed[i:i + step, :] = (x * lax.rsqrt(mean_sq + NORM_EPS) * gain[...].astype(F32)).astype(BF16)

    pl.semaphore_wait(barrier, group - 1)
    sends = [pltpu.make_async_remote_copy(
        src_ref=mine, dst_ref=held.at[k], send_sem=send_sem.at[k], recv_sem=recv_sem.at[k],
        device_id={"ep": peers[k]}, device_id_type=pl.DeviceIdType.MESH) for k in range(1, group)]
    for copy in sends:
        copy.start()

    logits = lax.dot_general(w_router_t[...], normed[...], (((1,), (1,)), ((), ())), preferred_element_type=F32)
    tot0 = jnp.sum(hit0, axis=1, keepdims=True)
    parts = []
    for i in range(0, tok, step):
        before = (lax.broadcasted_iota(jnp.int32, (tok, step), 0)
                  < i + lax.broadcasted_iota(jnp.int32, (tok, step), 1)).astype(F32).astype(BF16)
        parts.append(jnp.dot(both, before, preferred_element_type=F32))
    seen = jnp.concatenate(parts, axis=1)
    place = jnp.where(hit0 > 0, seen[:experts], jnp.where(hit1 > 0, seen[experts:] + tot0, -1.0))
    queue[...] = place.astype(jnp.int32)

    code = jnp.where(place < float(cap), eye.astype(F32) * float(cap) + place, -1.0)
    l0 = jnp.sum(hit0 * logits, axis=0, keepdims=True)
    l1 = jnp.sum(hit1 * logits, axis=0, keepdims=True)
    top = jnp.maximum(l0, l1)
    e0, e1 = jnp.exp(l0 - top), jnp.exp(l1 - top)
    lines = jnp.concatenate([jnp.sum(hit0 * code, axis=0, keepdims=True), jnp.sum(hit1 * code, axis=0, keepdims=True),
                             e0 / (e0 + e1), e1 / (e0 + e1), jnp.zeros((4, tok), F32)], axis=0)
    meta[...] = lines.T
    emit_packs(cap, normed, queue, [per * peers[2], per * peers[3]], far0, slots, sem)

    table[...] = jnp.zeros_like(table)
    table[0:1, :] = mine[0:1, :]
    for k, copy in enumerate(sends):
        copy.wait()
        table[k + 1:k + 2, :] = held[k + 1, 0:1, :]


def route(hidden, idst, gain, w_router_t, group, cap):
    tok, width = hidden.shape
    experts = w_router_t.shape[0]
    one = jax.ShapeDtypeStruct((cap, width), BF16)
    return pl.pallas_call(
        functools.partial(route_kernel, group, experts // group, cap),
        out_shape=[jax.ShapeDtypeStruct((tok, width), BF16), jax.ShapeDtypeStruct((experts, tok), jnp.int32),
                   jax.ShapeDtypeStruct((tok, 8), F32), jax.ShapeDtypeStruct((8, 128), jnp.int32), one, one],
        in_specs=[VMEM] * 4,
        out_specs=[VMEM] * 4 + [HBM] * 2,
        scratch_shapes=[pltpu.VMEM((2, cap, width), BF16), pltpu.SemaphoreType.DMA((2,)),
                        pltpu.VMEM((8, 128), jnp.int32), pltpu.VMEM((group, 8, 128), jnp.int32),
                        pltpu.SemaphoreType.DMA((group,)), pltpu.SemaphoreType.DMA((group,))],
        cost_estimate=pl.CostEstimate(flops=10**10, bytes_accessed=2 * 10**7, transcendentals=0),
        compiler_params=pltpu.CompilerParams(collective_id=0, has_side_effects=True, vmem_limit_bytes=62 * MIB),
    )(hidden, idst, gain, w_router_t)


def pack_kernel(group, per, cap, pairs, normed, queue, *rest):
    outs, (slots, sem) = rest[:len(pairs)], rest[len(pairs):]
    peers = peers_of(group)
    emit_packs(cap, normed, queue, [per * peers[k] + i for k, i in pairs], outs, slots, sem)


def pack(pairs, normed, queue, group, cap):
    _, width = normed.shape
    n = len(pairs)
    return pl.pallas_call(
        functools.partial(pack_kernel, group, queue.shape[0] // group, cap, pairs),
        out_shape=[jax.ShapeDtypeStruct((cap, width), BF16)] * n,
        in_specs=[VMEM] * 2,
        out_specs=[HBM] * n,
        scratch_shapes=[pltpu.VMEM((n, cap, width), BF16), pltpu.SemaphoreType.DMA((n,))],
        cost_estimate=pl.CostEstimate(flops=9 * 10**9, bytes_accessed=2 * 10**7, transcendentals=0),
        compiler_params=pltpu.CompilerParams(vmem_limit_bytes=62 * MIB),
    )(normed, queue)


def ffn_kernel(local, per, dist, cap, sizes, table, x0, x1, wg, wu, wd, o0, o1, xs, acc, bg, bu, bd, wsem, sem):
    steps = wg.shape[2] // TF
    expert = per * lax.axis_index("ep") + local
    n0 = pl.multiple_of((table[dist, expert] + BLK - 1) // BLK * BLK, BLK)
    rows = n0 + table[dist + 1, expert]

    def copies(f, slot):
        cols = pl.ds(pl.multiple_of(f * TF, TF), TF)
        return (pltpu.make_async_copy(wg.at[local, :, cols], bg.at[slot], wsem.at[0, slot]),
                pltpu.make_async_copy(wu.at[local, :, cols], bu.at[slot], wsem.at[1, slot]),
                pltpu.make_async_copy(wd.at[local, cols, :], bd.at[slot], wsem.at[2, slot]))

    def fetch(f, slot):
        for c in copies(f, slot):
            c.start()

    first = pltpu.make_async_copy(x0, xs.at[pl.ds(0, cap)], sem.at[0])
    first.start()
    fetch(0, 0)
    first.wait()
    second = pltpu.make_async_copy(x1, xs.at[pl.ds(n0, cap)], sem.at[1])
    second.start()
    acc[...] = jnp.zeros_like(acc)
    second.wait()

    def step(f, _):
        slot = lax.rem(f, NBUF)
        for c in copies(f, slot):
            c.wait()

        @pl.when(f == 0)
        def _():
            for k in range(1, NBUF - 1):
                fetch(k, k)

        @pl.when(f + NBUF - 1 < steps)
        def _():
            fetch(f + NBUF - 1, lax.rem(f + NBUF - 1, NBUF))

        def tile(m):
            x = xs[0:m, :]
            g = jnp.dot(x, bg[slot], preferred_element_type=F32)
            u = jnp.dot(x, bu[slot], preferred_element_type=F32)
            a = (jax.nn.silu(g) * u).astype(BF16)
            acc[0:m, :] += jnp.dot(a, bd[slot], preferred_element_type=F32)

        low = 0
        for m in sizes:
            @pl.when((rows > low) & (rows <= m))
            def _():
                tile(m)

            low = m
        return 0

    lax.fori_loop(0, steps, step, 0)
    xs[...] = acc[...].astype(BF16)
    a = pltpu.make_async_copy(xs.at[pl.ds(0, cap)], o0, sem.at[0])
    b = pltpu.make_async_copy(xs.at[pl.ds(n0, cap)], o1, sem.at[1])
    a.start()
    b.start()
    a.wait()
    b.wait()


def ffn(table, xs, wg, wu, wd, local, dist, cap):
    width, inner = wg.shape[1:]
    sizes = tuple(2 * cap - back for back in (192, 160, 128, 96, 64, 0))
    return pl.pallas_call(
        functools.partial(ffn_kernel, local, wg.shape[0], dist, cap, sizes),
        out_shape=[jax.ShapeDtypeStruct(x.shape, BF16) for x in xs],
        in_specs=[SMEM] + [ANY] * (3 + len(xs)),
        out_specs=[HBM] * len(xs),
        scratch_shapes=[pltpu.VMEM((2 * cap, width), BF16), pltpu.VMEM((2 * cap, width), F32),
                        pltpu.VMEM((NBUF, width, TF), BF16), pltpu.VMEM((NBUF, width, TF), BF16),
                        pltpu.VMEM((NBUF, TF, width), BF16),
                        pltpu.SemaphoreType.DMA((3, NBUF)), pltpu.SemaphoreType.DMA((2,))],
        cost_estimate=pl.CostEstimate(flops=6 * 540 * width * inner, bytes_accessed=6 * width * inner, transcendentals=0),
        compiler_params=pltpu.CompilerParams(vmem_limit_bytes=62 * MIB),
    )(table, *xs, wg, wu, wd)


def merge_kernel(group, per, cap, pairs, final, meta, *refs):
    extra, refs = refs[:2 * final], refs[2 * final:]
    bufs, (out, held, tgt, sem) = refs[:len(pairs)], refs[len(pairs):]

    @pl.when(pl.program_id(0) == 0)
    def _():
        copies = [pltpu.make_async_copy(buf, held.at[pl.ds(j * cap, cap)], sem.at[j]) for j, buf in enumerate(bufs)]
        for copy in copies:
            copy.start()
        peers = peers_of(group)
        lane = lax.broadcasted_iota(jnp.int32, tgt.shape, 1)
        want = jnp.full(tgt.shape, -2, jnp.int32)
        for j, (k, i) in enumerate(pairs):
            expert = per * peers[k] + i
            want = jnp.where((lane >= j * cap) & (lane < (j + 1) * cap), expert * cap + lane - j * cap, want)
        tgt[...] = want.astype(F32)
        at = len(pairs) * cap
        if at < held.shape[0]:
            held[at:, :] = jnp.zeros((held.shape[0] - at, held.shape[1]), BF16)
        for copy in copies:
            copy.wait()

    total = None
    for s in range(2):
        pick = (meta[:, s:s + 1] == tgt[0:1, :]).astype(F32).astype(BF16)
        got = meta[:, s + 2:s + 3] * jnp.dot(pick, held[...], preferred_element_type=F32)
        total = got if total is None else total + got
    if final:
        total = extra[1][...].astype(F32) + (extra[0][...] + total)
    out[...] = total.astype(out.dtype)


def merge(pairs, meta, bufs, group, per, cap, partial=None, hidden=None):
    tok, width = meta.shape[0], bufs[0].shape[1]
    deep = up_to(len(pairs) * cap, 256)
    final = hidden is not None
    rows = 256
    tile = pl.BlockSpec((rows, width), lambda i: (i, 0))
    extra = [partial, hidden] if final else []
    return pl.pallas_call(
        functools.partial(merge_kernel, group, per, cap, pairs, final),
        out_shape=jax.ShapeDtypeStruct((tok, width), BF16 if final else F32),
        grid=(tok // rows,),
        in_specs=[pl.BlockSpec((rows, 8), lambda i: (i, 0))] + [tile] * len(extra) + [ANY] * len(bufs),
        out_specs=tile,
        scratch_shapes=[pltpu.VMEM((deep, width), BF16), pltpu.VMEM((8, deep), F32),
                        pltpu.SemaphoreType.DMA((len(bufs),))],
        cost_estimate=pl.CostEstimate(flops=4 * tok * deep * width, bytes_accessed=2 * 10**7, transcendentals=0),
        compiler_params=pltpu.CompilerParams(vmem_limit_bytes=62 * MIB),
    )(meta, *extra, *bufs)


def solution(mesh):
    token_spec = P(("dp", "ep"), None)
    expert_spec = P("ep", None, None)

    def local_block(hidden, expert_ids, norm_gain, w_router, w_gate, w_up, w_down):
        tok, width = hidden.shape
        experts = w_router.shape[1]
        per = w_gate.shape[0]
        group = experts // per
        cap = (5 * tok + 2 * experts - 1) // (2 * experts)

        def swap(x, k):
            return lax.ppermute(x, "ep", [(i, i ^ k) for i in range(group)])

        def after(x, *earlier):
            return lax.optimization_barrier((x, *earlier))[0]

        idst = expert_ids.T
        normed, queue, meta, table, *far0 = route(
            hidden, idst, norm_gain.reshape(1, width), w_router.T, group, cap)
        got0 = [swap(far0[0], 2), swap(far0[1], 3)]
        own0, sib0, own1, sib1, *far1 = pack(
            [(0, 0), (1, 0), (0, 1), (1, 1), (2, 1), (3, 1)], normed, queue, group, cap)
        sib0, sib1 = swap(sib0, 1), swap(sib1, 1)
        got1 = [swap(far1[0], 2), swap(far1[1], 3)]

        def run(i, k, xs, *earlier):
            return ffn(after(table, *earlier), xs, w_gate, w_up, w_down, i, k, cap)

        o_own0, o_sib0 = run(0, 0, [own0, sib0])
        o_far0 = run(0, 2, got0, o_own0)
        back0 = [swap(o_far0[0], 2), swap(o_far0[1], 3)]
        o_far1 = run(1, 2, got1, o_far0[0])
        back1 = [swap(o_far1[0], 2), swap(o_far1[1], 3)]
        o_own1, o_sib1 = run(1, 0, [own1, sib1], o_far1[0])
        sib_back0 = swap(after(o_sib0, o_far1[0]), 1)
        sib_back1 = swap(o_sib1, 1)

        def gather(pairs, bufs, **kw):
            return merge(pairs, meta, bufs, group, per, cap, **kw)

        partial = gather([(0, 0), (1, 0), (0, 1), (2, 0), (3, 0)], [o_own0, sib_back0, o_own1] + back0)
        return gather([(1, 1), (2, 1), (3, 1)], [sib_back1] + back1, partial=partial, hidden=hidden)

    return jax.shard_map(local_block, mesh=mesh,
                         in_specs=(token_spec, token_spec, P(None), P(None, None), expert_spec, expert_spec, expert_spec),
                         out_specs=token_spec, check_vma=False)
```

```python
import functools

import jax
import jax.numpy as jnp
from jax import lax
from jax.experimental import pallas as pl
from jax.experimental.pallas import tpu as pltpu
from jax.sharding import PartitionSpec as P


NORM_EPS = 1e-5
F32 = jnp.float32
BF16 = jnp.bfloat16
BLK = 16
NBUF = 3
TF = 512
ANY = pl.BlockSpec(memory_space=pl.ANY)
SMEM = pl.BlockSpec(memory_space=pltpu.SMEM)
VMEM = pl.BlockSpec(memory_space=pltpu.VMEM)
HBM = pl.BlockSpec(memory_space=pltpu.HBM)
MIB = 2**20


def up_to(n, m):
    return (n + m - 1) // m * m


def peers_of(group):
    me = lax.axis_index("ep")
    return [me, me + 1 - 2 * lax.rem(me, 2), lax.rem(me + 2, group), group - 1 - me]


def pack_rows(normed, queue, expert, cap):
    place = queue[pl.ds(expert, 1), :]
    rows = lax.broadcasted_iota(jnp.int32, (cap, place.shape[1]), 0)
    pick = (rows == place).astype(F32).astype(BF16)
    return jnp.dot(pick, normed, preferred_element_type=F32).astype(BF16)


def emit_packs(cap, normed, queue, experts_of, outs, slots, sem):
    copies = []
    for k, (expert, out) in enumerate(zip(experts_of, outs)):
        slots[k] = pack_rows(normed[...], queue, expert, cap)
        copies.append(pltpu.make_async_copy(slots.at[k], out, sem.at[k]))
        copies[-1].start()
    for copy in copies:
        copy.wait()


def route_kernel(group, per, cap, hid, idst, gain, w_router_t, normed, queue, meta, table, *rest):
    far0, (slots, sem, mine, held, send_sem, recv_sem) = rest[:2], rest[2:]
    peers = peers_of(group)
    barrier = pltpu.get_barrier_semaphore()
    for peer in peers[1:]:
        pl.semaphore_signal(barrier, inc=1, device_id={"ep": peer}, device_id_type=pl.DeviceIdType.MESH)

    tok = hid.shape[0]
    experts = w_router_t.shape[0]
    eye = lax.broadcasted_iota(jnp.int32, (experts, tok), 0)
    hit0 = (idst[0:1, :] == eye).astype(F32)
    hit1 = (idst[1:2, :] == eye).astype(F32)
    both = jnp.concatenate([hit0, hit1], axis=0).astype(BF16)
    total = lax.dot_general(jnp.ones((8, tok), BF16), (hit0 + hit1).astype(BF16), (((1,), (1,)), ((), ())),
                            preferred_element_type=F32)
    mine[...] = jnp.zeros_like(mine)
    mine[:, 0:experts] = jnp.minimum(total, float(cap)).astype(jnp.int32)

    step = 256
    for i in range(0, tok, step):
        x = hid[i:i + step, :].astype(F32)
        mean_sq = jnp.mean(x * x, axis=-1, keepdims=True)
        normed[i:i + step, :] = (x * lax.rsqrt(mean_sq + NORM_EPS) * gain[...].astype(F32).reshape(1, -1)).astype(BF16)

    pl.semaphore_wait(barrier, group - 1)
    sends = [pltpu.make_async_remote_copy(
        src_ref=mine, dst_ref=held.at[k], send_sem=send_sem.at[k], recv_sem=recv_sem.at[k],
        device_id={"ep": peers[k]}, device_id_type=pl.DeviceIdType.MESH) for k in range(1, group)]
    for copy in sends:
        copy.start()

    logits = lax.dot_general(w_router_t[...], normed[...], (((1,), (1,)), ((), ())), preferred_element_type=F32)
    tot0 = jnp.sum(hit0, axis=1, keepdims=True)
    parts = []
    for i in range(0, tok, step):
        before = (lax.broadcasted_iota(jnp.int32, (tok, step), 0)
                  < i + lax.broadcasted_iota(jnp.int32, (tok, step), 1)).astype(F32).astype(BF16)
        parts.append(jnp.dot(both, before, preferred_element_type=F32))
    seen = jnp.concatenate(parts, axis=1)
    place = jnp.where(hit0 > 0, seen[:experts], jnp.where(hit1 > 0, seen[experts:] + tot0, -1.0))
    queue[...] = place.astype(jnp.int32)

    code = jnp.where(place < float(cap), eye.astype(F32) * float(cap) + place, -1.0)
    l0 = jnp.sum(hit0 * logits, axis=0, keepdims=True)
    l1 = jnp.sum(hit1 * logits, axis=0, keepdims=True)
    top = jnp.maximum(l0, l1)
    e0, e1 = jnp.exp(l0 - top), jnp.exp(l1 - top)
    lines = jnp.concatenate([jnp.sum(hit0 * code, axis=0, keepdims=True), jnp.sum(hit1 * code, axis=0, keepdims=True),
                             e0 / (e0 + e1), e1 / (e0 + e1), jnp.zeros((4, tok), F32)], axis=0)
    meta[...] = lines.T
    emit_packs(cap, normed, queue, [per * peers[2], per * peers[3]], far0, slots, sem)

    table[...] = jnp.zeros_like(table)
    table[0:1, :] = mine[0:1, :]
    for k, copy in enumerate(sends):
        copy.wait()
        table[k + 1:k + 2, :] = held[k + 1, 0:1, :]


def route(hidden, idst, gain, w_router_t, group, cap):
    tok, width = hidden.shape
    experts = w_router_t.shape[0]
    one = jax.ShapeDtypeStruct((cap, width), BF16)
    return pl.pallas_call(
        functools.partial(route_kernel, group, experts // group, cap),
        out_shape=[jax.ShapeDtypeStruct((tok, width), BF16), jax.ShapeDtypeStruct((experts, tok), jnp.int32),
                   jax.ShapeDtypeStruct((tok, 8), F32), jax.ShapeDtypeStruct((8, 128), jnp.int32), one, one],
        in_specs=[VMEM] * 4,
        out_specs=[VMEM] * 4 + [HBM] * 2,
        scratch_shapes=[pltpu.VMEM((2, cap, width), BF16), pltpu.SemaphoreType.DMA((2,)),
                        pltpu.VMEM((8, 128), jnp.int32), pltpu.VMEM((group, 8, 128), jnp.int32),
                        pltpu.SemaphoreType.DMA((group,)), pltpu.SemaphoreType.DMA((group,))],
        cost_estimate=pl.CostEstimate(flops=10**10, bytes_accessed=2 * 10**7, transcendentals=0),
        compiler_params=pltpu.CompilerParams(collective_id=0, has_side_effects=True, vmem_limit_bytes=62 * MIB),
    )(hidden, idst, gain, w_router_t)


def pack_kernel(group, per, cap, pairs, normed, queue, *rest):
    outs, (slots, sem) = rest[:len(pairs)], rest[len(pairs):]
    peers = peers_of(group)
    emit_packs(cap, normed, queue, [per * peers[k] + i for k, i in pairs], outs, slots, sem)


def pack(pairs, normed, queue, group, cap):
    _, width = normed.shape
    n = len(pairs)
    return pl.pallas_call(
        functools.partial(pack_kernel, group, queue.shape[0] // group, cap, pairs),
        out_shape=[jax.ShapeDtypeStruct((cap, width), BF16)] * n,
        in_specs=[VMEM] * 2,
        out_specs=[HBM] * n,
        scratch_shapes=[pltpu.VMEM((n, cap, width), BF16), pltpu.SemaphoreType.DMA((n,))],
        cost_estimate=pl.CostEstimate(flops=9 * 10**9, bytes_accessed=2 * 10**7, transcendentals=0),
        compiler_params=pltpu.CompilerParams(vmem_limit_bytes=62 * MIB),
    )(normed, queue)


def ffn_kernel(local, per, dist, cap, sizes, table, x0, x1, wg, wu, wd, o0, o1, xs, acc, bg, bu, bd, wsem, sem):
    steps = wg.shape[2] // TF
    expert = per * lax.axis_index("ep") + local
    n0 = pl.multiple_of((table[dist, expert] + BLK - 1) // BLK * BLK, BLK)
    rows = n0 + table[dist + 1, expert]

    def copies(f, slot):
        cols = pl.ds(pl.multiple_of(f * TF, TF), TF)
        return (pltpu.make_async_copy(wg.at[local, :, cols], bg.at[slot], wsem.at[0, slot]),
                pltpu.make_async_copy(wu.at[local, :, cols], bu.at[slot], wsem.at[1, slot]),
                pltpu.make_async_copy(wd.at[local, cols, :], bd.at[slot], wsem.at[2, slot]))

    def fetch(f, slot):
        for c in copies(f, slot):
            c.start()

    first = pltpu.make_async_copy(x0, xs.at[pl.ds(0, cap)], sem.at[0])
    first.start()
    fetch(0, 0)
    first.wait()
    second = pltpu.make_async_copy(x1, xs.at[pl.ds(n0, cap)], sem.at[1])
    second.start()
    acc[...] = jnp.zeros_like(acc)
    second.wait()

    def step(f, _):
        slot = lax.rem(f, NBUF)
        for c in copies(f, slot):
            c.wait()

        @pl.when(f == 0)
        def _():
            for k in range(1, NBUF - 1):
                fetch(k, k)

        @pl.when(f + NBUF - 1 < steps)
        def _():
            fetch(f + NBUF - 1, lax.rem(f + NBUF - 1, NBUF))

        def tile(m):
            x = xs[0:m, :]
            g = jnp.dot(x, bg[slot], preferred_element_type=F32)
            u = jnp.dot(x, bu[slot], preferred_element_type=F32)
            a = (jax.nn.silu(g) * u).astype(BF16)
            acc[0:m, :] += jnp.dot(a, bd[slot], preferred_element_type=F32)

        low = 0
        for m in sizes:
            @pl.when((rows > low) & (rows <= m))
            def _():
                tile(m)

            low = m
        return 0

    lax.fori_loop(0, steps, step, 0)
    xs[...] = acc[...].astype(BF16)
    a = pltpu.make_async_copy(xs.at[pl.ds(0, cap)], o0, sem.at[0])
    b = pltpu.make_async_copy(xs.at[pl.ds(n0, cap)], o1, sem.at[1])
    a.start()
    b.start()
    a.wait()
    b.wait()


def ffn(table, xs, wg, wu, wd, local, dist, cap):
    width, inner = wg.shape[1:]
    sizes = tuple(2 * cap - back for back in (192, 160, 128, 96, 64, 0))
    return pl.pallas_call(
        functools.partial(ffn_kernel, local, wg.shape[0], dist, cap, sizes),
        out_shape=[jax.ShapeDtypeStruct(x.shape, BF16) for x in xs],
        in_specs=[SMEM] + [ANY] * (3 + len(xs)),
        out_specs=[HBM] * len(xs),
        scratch_shapes=[pltpu.VMEM((2 * cap, width), BF16), pltpu.VMEM((2 * cap, width), F32),
                        pltpu.VMEM((NBUF, width, TF), BF16), pltpu.VMEM((NBUF, width, TF), BF16),
                        pltpu.VMEM((NBUF, TF, width), BF16),
                        pltpu.SemaphoreType.DMA((3, NBUF)), pltpu.SemaphoreType.DMA((2,))],
        cost_estimate=pl.CostEstimate(flops=6 * 540 * width * inner, bytes_accessed=6 * width * inner, transcendentals=0),
        compiler_params=pltpu.CompilerParams(vmem_limit_bytes=62 * MIB),
    )(table, *xs, wg, wu, wd)


def merge_kernel(group, per, cap, pairs, final, meta, *refs):
    extra, refs = refs[:2 * final], refs[2 * final:]
    bufs, (out, held, tgt, sem) = refs[:len(pairs)], refs[len(pairs):]

    @pl.when(pl.program_id(0) == 0)
    def _():
        copies = [pltpu.make_async_copy(buf, held.at[pl.ds(j * cap, cap)], sem.at[j]) for j, buf in enumerate(bufs)]
        for copy in copies:
            copy.start()
        peers = peers_of(group)
        lane = lax.broadcasted_iota(jnp.int32, tgt.shape, 1)
        want = jnp.full(tgt.shape, -2, jnp.int32)
        for j, (k, i) in enumerate(pairs):
            expert = per * peers[k] + i
            want = jnp.where((lane >= j * cap) & (lane < (j + 1) * cap), expert * cap + lane - j * cap, want)
        tgt[...] = want.astype(F32)
        at = len(pairs) * cap
        if at < held.shape[0]:
            held[at:, :] = jnp.zeros((held.shape[0] - at, held.shape[1]), BF16)
        for copy in copies:
            copy.wait()

    total = None
    for s in range(2):
        pick = (meta[:, s:s + 1] == tgt[0:1, :]).astype(F32).astype(BF16)
        got = meta[:, s + 2:s + 3] * jnp.dot(pick, held[...], preferred_element_type=F32)
        total = got if total is None else total + got
    if final:
        total = extra[1][...].astype(F32) + (extra[0][...] + total)
    out[...] = total.astype(out.dtype)


def merge(pairs, meta, bufs, group, per, cap, partial=None, hidden=None):
    tok, width = meta.shape[0], bufs[0].shape[1]
    deep = up_to(len(pairs) * cap, 256)
    final = hidden is not None
    rows = 256
    tile = pl.BlockSpec((rows, width), lambda i: (i, 0))
    extra = [partial, hidden] if final else []
    return pl.pallas_call(
        functools.partial(merge_kernel, group, per, cap, pairs, final),
        out_shape=jax.ShapeDtypeStruct((tok, width), BF16 if final else F32),
        grid=(tok // rows,),
        in_specs=[pl.BlockSpec((rows, 8), lambda i: (i, 0))] + [tile] * len(extra) + [ANY] * len(bufs),
        out_specs=tile,
        scratch_shapes=[pltpu.VMEM((deep, width), BF16), pltpu.VMEM((8, deep), F32),
                        pltpu.SemaphoreType.DMA((len(bufs),))],
        cost_estimate=pl.CostEstimate(flops=4 * tok * deep * width, bytes_accessed=2 * 10**7, transcendentals=0),
        compiler_params=pltpu.CompilerParams(vmem_limit_bytes=62 * MIB),
    )(meta, *extra, *bufs)


def solution(mesh):
    token_spec = P(("dp", "ep"), None)
    expert_spec = P("ep", None, None)

    def local_block(hidden, expert_ids, norm_gain, w_router, w_gate, w_up, w_down):
        tok, _ = hidden.shape
        experts = w_router.shape[1]
        per = w_gate.shape[0]
        group = experts // per
        cap = (5 * tok + 2 * experts - 1) // (2 * experts)

        def swap(x, k):
            return lax.ppermute(x, "ep", [(i, i ^ k) for i in range(group)])

        def after(x, *earlier):
            return lax.optimization_barrier((x, *earlier))[0]

        idst = expert_ids.T
        normed, queue, meta, table, *far0 = route(
            hidden, idst, norm_gain, w_router.T, group, cap)
        got0 = [swap(far0[0], 2), swap(far0[1], 3)]
        own0, sib0, *far1 = pack([(0, 0), (1, 0), (2, 1), (3, 1)], normed, queue, group, cap)
        sib0 = swap(sib0, 1)
        got1 = [swap(far1[0], 2), swap(far1[1], 3)]

        def run(i, k, xs, *earlier):
            return ffn(after(table, *earlier), xs, w_gate, w_up, w_down, i, k, cap)

        o_own0, o_sib0 = run(0, 0, [own0, sib0])
        o_far0 = run(0, 2, got0, o_own0)
        own1, sib1 = pack([(0, 1), (1, 1)], after(normed, o_far0[0]), queue, group, cap)
        sib1 = swap(sib1, 1)
        back0 = [swap(after(o_far0[j], *got1), 2 + j) for j in range(2)]
        o_far1 = run(1, 2, got1, o_far0[0], own1)
        back1 = [swap(o_far1[0], 2), swap(o_far1[1], 3)]
        o_own1, o_sib1 = run(1, 0, [own1, sib1], o_far1[0])
        sib_back0 = swap(after(o_sib0, o_far1[0]), 1)
        sib_back1 = swap(o_sib1, 1)

        def gather(pairs, bufs, **kw):
            return merge(pairs, meta, bufs, group, per, cap, **kw)

        partial = gather([(0, 0), (1, 0), (0, 1), (1, 1), (2, 0), (3, 0)],
                         [o_own0, sib_back0, o_own1, sib_back1] + back0)
        return gather([(2, 1), (3, 1)], back1, partial=partial, hidden=hidden)

    return jax.shard_map(local_block, mesh=mesh,
                         in_specs=(token_spec, token_spec, P(None), P(None, None), expert_spec, expert_spec, expert_spec),
                         out_specs=token_spec, check_vma=False)
```

```python
import functools

import jax
import jax.numpy as jnp
from jax import lax
from jax.experimental import pallas as pl
from jax.experimental.pallas import tpu as pltpu
from jax.sharding import PartitionSpec as P


NORM_EPS = 1e-5
F32 = jnp.float32
BF16 = jnp.bfloat16
BLK = 16
NBUF = 3
TF = 512
ANY = pl.BlockSpec(memory_space=pl.ANY)
SMEM = pl.BlockSpec(memory_space=pltpu.SMEM)
VMEM = pl.BlockSpec(memory_space=pltpu.VMEM)
HBM = pl.BlockSpec(memory_space=pltpu.HBM)
MIB = 2**20


def peers_of(group):
    me = lax.axis_index("ep")
    return [me, me + 1 - 2 * lax.rem(me, 2), lax.rem(me + 2, group), group - 1 - me]


def pack_rows(normed, queue, expert, cap):
    place = queue[pl.ds(expert, 1), :]
    rows = lax.broadcasted_iota(jnp.int32, (cap, place.shape[1]), 0)
    pick = (rows == place).astype(F32).astype(BF16)
    return jnp.dot(pick, normed, preferred_element_type=F32).astype(BF16)


def emit_packs(cap, normed, queue, experts_of, outs, slots, sem):
    copies = []
    for k, (expert, out) in enumerate(zip(experts_of, outs)):
        slots[k] = pack_rows(normed[...], queue, expert, cap)
        copies.append(pltpu.make_async_copy(slots.at[k], out, sem.at[k]))
        copies[-1].start()
    for copy in copies:
        copy.wait()


def route_kernel(group, per, cap, hid_hbm, idst, gain, w_router_t, normed_hbm, queue, meta, table, *rest):
    far0, (hid, normed, row_sem, slots, sem, mine, held, send_sem, recv_sem) = rest[:2], rest[2:]
    tok = hid.shape[0]
    step = 256
    loads = [pltpu.make_async_copy(hid_hbm.at[pl.ds(i, step)], hid.at[pl.ds(i, step)], row_sem.at[i // step])
             for i in range(0, tok, step)]
    for copy in loads:
        copy.start()
    peers = peers_of(group)
    barrier = pltpu.get_barrier_semaphore()
    for peer in peers[1:]:
        pl.semaphore_signal(barrier, inc=1, device_id={"ep": peer}, device_id_type=pl.DeviceIdType.MESH)

    experts = w_router_t.shape[0]
    eye = lax.broadcasted_iota(jnp.int32, (experts, tok), 0)
    hit0 = (idst[0:1, :] == eye).astype(F32)
    hit1 = (idst[1:2, :] == eye).astype(F32)
    both = jnp.concatenate([hit0, hit1], axis=0).astype(BF16)
    total = lax.dot_general(jnp.ones((8, tok), BF16), (hit0 + hit1).astype(BF16), (((1,), (1,)), ((), ())),
                            preferred_element_type=F32)
    mine[...] = jnp.zeros_like(mine)
    mine[:, 0:experts] = jnp.minimum(total, float(cap)).astype(jnp.int32)

    for i in range(0, tok, step):
        loads[i // step].wait()
        x = hid[i:i + step, :].astype(F32)
        mean_sq = jnp.mean(x * x, axis=-1, keepdims=True)
        normed[i:i + step, :] = (x * lax.rsqrt(mean_sq + NORM_EPS) * gain[...].astype(F32).reshape(1, -1)).astype(BF16)

    keep = pltpu.make_async_copy(normed, normed_hbm, row_sem.at[tok // step])
    keep.start()
    pl.semaphore_wait(barrier, group - 1)
    sends = [pltpu.make_async_remote_copy(
        src_ref=mine, dst_ref=held.at[k], send_sem=send_sem.at[k], recv_sem=recv_sem.at[k],
        device_id={"ep": peers[k]}, device_id_type=pl.DeviceIdType.MESH) for k in range(1, group)]
    for copy in sends:
        copy.start()

    logits = lax.dot_general(w_router_t[...], normed[...], (((1,), (1,)), ((), ())), preferred_element_type=F32)
    tot0 = jnp.sum(hit0, axis=1, keepdims=True)
    parts = []
    for i in range(0, tok, step):
        before = (lax.broadcasted_iota(jnp.int32, (tok, step), 0)
                  < i + lax.broadcasted_iota(jnp.int32, (tok, step), 1)).astype(F32).astype(BF16)
        parts.append(jnp.dot(both, before, preferred_element_type=F32))
    seen = jnp.concatenate(parts, axis=1)
    place = jnp.where(hit0 > 0, seen[:experts], jnp.where(hit1 > 0, seen[experts:] + tot0, -1.0))
    queue[...] = place.astype(jnp.int32)

    code = jnp.where(place < float(cap), eye.astype(F32) * float(cap) + place, -1.0)
    l0 = jnp.sum(hit0 * logits, axis=0, keepdims=True)
    l1 = jnp.sum(hit1 * logits, axis=0, keepdims=True)
    top = jnp.maximum(l0, l1)
    e0, e1 = jnp.exp(l0 - top), jnp.exp(l1 - top)
    lines = jnp.concatenate([jnp.sum(hit0 * code, axis=0, keepdims=True), jnp.sum(hit1 * code, axis=0, keepdims=True),
                             e0 / (e0 + e1), e1 / (e0 + e1), jnp.zeros((4, tok), F32)], axis=0)
    meta[...] = lines.T
    emit_packs(cap, normed, queue, [per * peers[2], per * peers[3]], far0, slots, sem)

    keep.wait()
    table[...] = jnp.zeros_like(table)
    table[0:1, :] = mine[0:1, :]
    for k, copy in enumerate(sends):
        copy.wait()
        table[k + 1:k + 2, :] = held[k + 1, 0:1, :]


def route(hidden, idst, gain, w_router_t, group, cap):
    tok, width = hidden.shape
    experts = w_router_t.shape[0]
    one = jax.ShapeDtypeStruct((cap, width), BF16)
    return pl.pallas_call(
        functools.partial(route_kernel, group, experts // group, cap),
        out_shape=[jax.ShapeDtypeStruct((tok, width), BF16), jax.ShapeDtypeStruct((experts, tok), jnp.int32),
                   jax.ShapeDtypeStruct((tok, 8), F32), jax.ShapeDtypeStruct((8, 128), jnp.int32), one, one],
        in_specs=[HBM] + [VMEM] * 3,
        out_specs=[HBM] + [VMEM] * 3 + [HBM] * 2,
        scratch_shapes=[pltpu.VMEM((tok, width), BF16), pltpu.VMEM((tok, width), BF16), pltpu.SemaphoreType.DMA((5,)),
                        pltpu.VMEM((2, cap, width), BF16), pltpu.SemaphoreType.DMA((2,)),
                        pltpu.VMEM((8, 128), jnp.int32), pltpu.VMEM((group, 8, 128), jnp.int32),
                        pltpu.SemaphoreType.DMA((group,)), pltpu.SemaphoreType.DMA((group,))],
        cost_estimate=pl.CostEstimate(flops=10**10, bytes_accessed=2 * 10**7, transcendentals=0),
        compiler_params=pltpu.CompilerParams(collective_id=0, has_side_effects=True, vmem_limit_bytes=62 * MIB),
    )(hidden, idst, gain, w_router_t)


def pack_kernel(group, per, cap, pairs, normed, queue, *rest):
    outs, (slots, sem) = rest[:len(pairs)], rest[len(pairs):]
    peers = peers_of(group)
    emit_packs(cap, normed, queue, [per * peers[k] + i for k, i in pairs], outs, slots, sem)


def pack(pairs, normed, queue, group, cap):
    _, width = normed.shape
    n = len(pairs)
    return pl.pallas_call(
        functools.partial(pack_kernel, group, queue.shape[0] // group, cap, pairs),
        out_shape=[jax.ShapeDtypeStruct((cap, width), BF16)] * n,
        in_specs=[VMEM] * 2,
        out_specs=[HBM] * n,
        scratch_shapes=[pltpu.VMEM((n, cap, width), BF16), pltpu.SemaphoreType.DMA((n,))],
        cost_estimate=pl.CostEstimate(flops=9 * 10**9, bytes_accessed=2 * 10**7, transcendentals=0),
        compiler_params=pltpu.CompilerParams(vmem_limit_bytes=62 * MIB),
    )(normed, queue)


def ffn_kernel(local, per, dist, cap, sizes, table, x0, x1, wg, wu, wd, o0, o1, xs, acc, bg, bu, bd, wsem, sem):
    steps = wg.shape[2] // TF
    expert = per * lax.axis_index("ep") + local
    n0 = pl.multiple_of((table[dist, expert] + BLK - 1) // BLK * BLK, BLK)
    rows = n0 + table[dist + 1, expert]

    def copies(f, slot):
        cols = pl.ds(pl.multiple_of(f * TF, TF), TF)
        return (pltpu.make_async_copy(wg.at[local, :, cols], bg.at[slot], wsem.at[0, slot]),
                pltpu.make_async_copy(wu.at[local, :, cols], bu.at[slot], wsem.at[1, slot]),
                pltpu.make_async_copy(wd.at[local, cols, :], bd.at[slot], wsem.at[2, slot]))

    def fetch(f, slot):
        for c in copies(f, slot):
            c.start()

    first = pltpu.make_async_copy(x0, xs.at[pl.ds(0, cap)], sem.at[0])
    first.start()
    fetch(0, 0)
    first.wait()
    second = pltpu.make_async_copy(x1, xs.at[pl.ds(n0, cap)], sem.at[1])
    second.start()
    acc[...] = jnp.zeros_like(acc)
    second.wait()

    def step(f, _):
        slot = lax.rem(f, NBUF)
        for c in copies(f, slot):
            c.wait()

        @pl.when(f == 0)
        def _():
            for k in range(1, NBUF - 1):
                fetch(k, k)

        @pl.when(f + NBUF - 1 < steps)
        def _():
            fetch(f + NBUF - 1, lax.rem(f + NBUF - 1, NBUF))

        def tile(m):
            x = xs[0:m, :]
            g = jnp.dot(x, bg[slot], preferred_element_type=F32)
            u = jnp.dot(x, bu[slot], preferred_element_type=F32)
            a = (jax.nn.silu(g) * u).astype(BF16)
            acc[0:m, :] += jnp.dot(a, bd[slot], preferred_element_type=F32)

        low = 0
        for m in sizes:
            @pl.when((rows > low) & (rows <= m))
            def _():
                tile(m)

            low = m
        return 0

    lax.fori_loop(0, steps, step, 0)
    xs[...] = acc[...].astype(BF16)
    a = pltpu.make_async_copy(xs.at[pl.ds(0, cap)], o0, sem.at[0])
    b = pltpu.make_async_copy(xs.at[pl.ds(n0, cap)], o1, sem.at[1])
    a.start()
    b.start()
    a.wait()
    b.wait()


def ffn(table, xs, wg, wu, wd, local, dist, cap):
    width, inner = wg.shape[1:]
    sizes = tuple(2 * cap - back for back in (192, 160, 128, 96, 64, 0))
    return pl.pallas_call(
        functools.partial(ffn_kernel, local, wg.shape[0], dist, cap, sizes),
        out_shape=[jax.ShapeDtypeStruct(x.shape, BF16) for x in xs],
        in_specs=[SMEM] + [ANY] * (3 + len(xs)),
        out_specs=[HBM] * len(xs),
        scratch_shapes=[pltpu.VMEM((2 * cap, width), BF16), pltpu.VMEM((2 * cap, width), F32),
                        pltpu.VMEM((NBUF, width, TF), BF16), pltpu.VMEM((NBUF, width, TF), BF16),
                        pltpu.VMEM((NBUF, TF, width), BF16),
                        pltpu.SemaphoreType.DMA((3, NBUF)), pltpu.SemaphoreType.DMA((2,))],
        cost_estimate=pl.CostEstimate(flops=6 * 540 * width * inner, bytes_accessed=6 * width * inner, transcendentals=0),
        compiler_params=pltpu.CompilerParams(vmem_limit_bytes=62 * MIB),
    )(table, *xs, wg, wu, wd)


def merge_kernel(group, per, cap, pairs, meta, hid, *refs):
    bufs, (out, held, tgt, sem) = refs[:len(pairs)], refs[len(pairs):]
    half = len(pairs) // 2
    cut = half * cap
    first = pl.program_id(0) == 0

    def copy(j):
        return pltpu.make_async_copy(bufs[j], held.at[pl.ds(j * cap, cap)], sem.at[j])

    @pl.when(first)
    def _():
        for j in range(len(pairs)):
            copy(j).start()
        peers = peers_of(group)
        lane = lax.broadcasted_iota(jnp.int32, tgt.shape, 1)
        want = jnp.full(tgt.shape, -2, jnp.int32)
        for j, (k, i) in enumerate(pairs):
            expert = per * peers[k] + i
            want = jnp.where((lane >= j * cap) & (lane < (j + 1) * cap), expert * cap + lane - j * cap, want)
        tgt[...] = want.astype(F32)
        for j in range(half):
            copy(j).wait()

    def fetch(lo, hi):
        pick = jnp.concatenate([(meta[:, s:s + 1] == tgt[0:1, lo:hi]).astype(F32).astype(BF16) for s in range(2)], axis=0)
        return jnp.dot(pick, held[lo:hi, :], preferred_element_type=F32)

    rows = meta.shape[0]
    got = fetch(0, cut)
    near = meta[:, 2:3] * got[:rows] + meta[:, 3:4] * got[rows:]

    @pl.when(first)
    def _():
        for j in range(half, len(pairs)):
            copy(j).wait()

    got = fetch(cut, 2 * cut)
    far = meta[:, 2:3] * got[:rows] + meta[:, 3:4] * got[rows:]
    out[...] = (hid[...].astype(F32) + (near + far)).astype(out.dtype)


def merge(pairs, meta, hidden, bufs, group, per, cap):
    tok, width = hidden.shape
    deep = len(pairs) * cap
    rows = 256
    tile = pl.BlockSpec((rows, width), lambda i: (i, 0))
    return pl.pallas_call(
        functools.partial(merge_kernel, group, per, cap, pairs),
        out_shape=jax.ShapeDtypeStruct((tok, width), BF16),
        grid=(tok // rows,),
        in_specs=[pl.BlockSpec((rows, 8), lambda i: (i, 0)), tile] + [ANY] * len(bufs),
        out_specs=tile,
        scratch_shapes=[pltpu.VMEM((deep, width), BF16), pltpu.VMEM((8, deep), F32),
                        pltpu.SemaphoreType.DMA((len(bufs),))],
        cost_estimate=pl.CostEstimate(flops=4 * tok * deep * width, bytes_accessed=2 * 10**7, transcendentals=0),
        compiler_params=pltpu.CompilerParams(vmem_limit_bytes=62 * MIB),
    )(meta, hidden, *bufs)


def solution(mesh):
    token_spec = P(("dp", "ep"), None)
    expert_spec = P("ep", None, None)

    def local_block(hidden, expert_ids, norm_gain, w_router, w_gate, w_up, w_down):
        tok, _ = hidden.shape
        experts = w_router.shape[1]
        per = w_gate.shape[0]
        group = experts // per
        cap = (5 * tok + 2 * experts - 1) // (2 * experts)

        def swap(x, k):
            return lax.ppermute(x, "ep", [(i, i ^ k) for i in range(group)])

        def after(x, *earlier):
            return lax.optimization_barrier((x, *earlier))[0]

        idst = expert_ids.T
        normed, queue, meta, table, *far0 = route(
            hidden, idst, norm_gain, w_router.T, group, cap)
        got0 = [swap(far0[0], 2), swap(far0[1], 3)]
        own0, sib0, *far1 = pack([(0, 0), (1, 0), (2, 1), (3, 1)], normed, queue, group, cap)
        sib0 = swap(sib0, 1)
        got1 = [swap(far1[0], 2), swap(far1[1], 3)]

        def run(i, k, xs, *earlier):
            return ffn(after(table, *earlier), xs, w_gate, w_up, w_down, i, k, cap)

        o_own0, o_sib0 = run(0, 0, [own0, sib0])
        o_far0 = run(0, 2, got0, o_own0)
        own1, sib1 = pack([(0, 1), (1, 1)], after(normed, o_far0[0]), queue, group, cap)
        sib1 = swap(sib1, 1)
        back0 = [swap(after(o_far0[j], *got1), 2 + j) for j in range(2)]
        o_far1 = run(1, 2, got1, o_far0[0], own1)
        back1 = [swap(o_far1[0], 2), swap(o_far1[1], 3)]
        o_own1, o_sib1 = run(1, 0, [own1, sib1], o_far1[0])
        sib_back0 = swap(after(o_sib0, o_far1[0]), 1)
        sib_back1 = swap(o_sib1, 1)

        return merge([(0, 0), (0, 1), (1, 0), (1, 1), (2, 0), (3, 0), (2, 1), (3, 1)], meta, hidden,
                     [o_own0, o_own1, sib_back0, sib_back1] + back0 + back1, group, per, cap)

    return jax.shard_map(local_block, mesh=mesh,
                         in_specs=(token_spec, token_spec, P(None), P(None, None), expert_spec, expert_spec, expert_spec),
                         out_specs=token_spec, check_vma=False)
```

```python
import functools

import jax
import jax.numpy as jnp
from jax import lax
from jax.experimental import pallas as pl
from jax.experimental.pallas import tpu as pltpu
from jax.sharding import PartitionSpec as P


NORM_EPS = 1e-5
F32 = jnp.float32
BF16 = jnp.bfloat16
BLK = 16
TAIL = 48
NBUF = 3
TF = 512
ANY = pl.BlockSpec(memory_space=pl.ANY)
SMEM = pl.BlockSpec(memory_space=pltpu.SMEM)
VMEM = pl.BlockSpec(memory_space=pltpu.VMEM)
HBM = pl.BlockSpec(memory_space=pltpu.HBM)
MIB = 2**20


def up_to(n, m):
    return (n + m - 1) // m * m


def peers_of(group):
    me = lax.axis_index("ep")
    return [me, me + 1 - 2 * lax.rem(me, 2), lax.rem(me + 2, group), group - 1 - me]


def pack_rows(normed, queue, wanted, lo, count):
    rows = lo + lax.broadcasted_iota(jnp.int32, (count, queue.shape[1]), 0)
    hit, shift = None, None
    for expert in wanted:
        place = queue[pl.ds(expert, 1), :]
        kept = place >= 0
        at = place if shift is None else jnp.where(kept, place + shift, -1)
        here = rows == at
        hit = here if hit is None else hit | here
        held = jnp.sum(kept.astype(F32), axis=1, keepdims=True).astype(jnp.int32)
        shift = (held + (BLK - 1)) // BLK * BLK
    return jnp.dot(hit.astype(F32).astype(BF16), normed, preferred_element_type=F32).astype(BF16)


def emit_packs(cap, normed, queue, jobs, outs, slots, sem):
    copies = []
    outs = list(outs)
    for k, (wanted, lo) in enumerate(jobs):
        slots[k] = pack_rows(normed[...], queue, wanted, lo, cap)
        at = 0
        while at < cap:
            out = outs.pop(0)
            copies.append(pltpu.make_async_copy(slots.at[k, pl.ds(at, out.shape[0])], out, sem.at[len(copies)]))
            copies[-1].start()
            at += out.shape[0]
    for copy in copies:
        copy.wait()


def route_kernel(group, per, cap, hid_hbm, idst, gain, w_router_t, normed_hbm, queue, meta, table, *rest):
    far0, (hid, normed, row_sem, slots, sem, mine, held, send_sem, recv_sem) = rest[:2], rest[2:]
    tok = hid.shape[0]
    step = 256
    loads = [pltpu.make_async_copy(hid_hbm.at[pl.ds(i, step)], hid.at[pl.ds(i, step)], row_sem.at[i // step])
             for i in range(0, tok, step)]
    for copy in loads:
        copy.start()
    peers = peers_of(group)
    other = 1 - lax.axis_index("dp")
    mates = [{"ep": peer} for peer in peers[1:]] + [{"dp": other, "ep": peer} for peer in peers]
    barrier = pltpu.get_barrier_semaphore()
    for mate in mates:
        pl.semaphore_signal(barrier, inc=1, device_id=mate, device_id_type=pl.DeviceIdType.MESH)

    experts = w_router_t.shape[0]
    eye = lax.broadcasted_iota(jnp.int32, (experts, tok), 0)
    hit0 = (idst[0:1, :] == eye).astype(F32)
    hit1 = (idst[1:2, :] == eye).astype(F32)
    both = jnp.concatenate([hit0, hit1], axis=0).astype(BF16)
    total = lax.dot_general(jnp.ones((8, tok), BF16), (hit0 + hit1).astype(BF16), (((1,), (1,)), ((), ())),
                            preferred_element_type=F32)
    mine[...] = jnp.zeros_like(mine)
    mine[:, 0:experts] = jnp.minimum(total, float(cap)).astype(jnp.int32)

    for i in range(0, tok, step):
        loads[i // step].wait()
        x = hid[i:i + step, :].astype(F32)
        mean_sq = jnp.mean(x * x, axis=-1, keepdims=True)
        normed[i:i + step, :] = (x * lax.rsqrt(mean_sq + NORM_EPS) * gain[...].astype(F32).reshape(1, -1)).astype(BF16)

    keep = pltpu.make_async_copy(normed, normed_hbm, row_sem.at[tok // step])
    keep.start()
    pl.semaphore_wait(barrier, len(mates))
    sends = [pltpu.make_async_remote_copy(
        src_ref=mine, dst_ref=held.at[k], send_sem=send_sem.at[k], recv_sem=recv_sem.at[k],
        device_id=mate, device_id_type=pl.DeviceIdType.MESH) for k, mate in enumerate(mates)]
    for copy in sends:
        copy.start()

    logits = lax.dot_general(w_router_t[...], normed[...], (((1,), (1,)), ((), ())), preferred_element_type=F32)
    tot0 = jnp.sum(hit0, axis=1, keepdims=True)
    parts = []
    for i in range(0, tok, step):
        before = (lax.broadcasted_iota(jnp.int32, (tok, step), 0)
                  < i + lax.broadcasted_iota(jnp.int32, (tok, step), 1)).astype(F32).astype(BF16)
        parts.append(jnp.dot(both, before, preferred_element_type=F32))
    seen = jnp.concatenate(parts, axis=1)
    place = jnp.where(hit0 > 0, seen[:experts], jnp.where(hit1 > 0, seen[experts:] + tot0, -1.0))
    queue[...] = jnp.where(place < float(cap), place, -1.0).astype(jnp.int32)

    code = jnp.where(place < float(cap), eye.astype(F32) * float(cap) + place, -1.0)
    l0 = jnp.sum(hit0 * logits, axis=0, keepdims=True)
    l1 = jnp.sum(hit1 * logits, axis=0, keepdims=True)
    top = jnp.maximum(l0, l1)
    e0, e1 = jnp.exp(l0 - top), jnp.exp(l1 - top)
    lines = jnp.concatenate([jnp.sum(hit0 * code, axis=0, keepdims=True), jnp.sum(hit1 * code, axis=0, keepdims=True),
                             e0 / (e0 + e1), e1 / (e0 + e1), jnp.zeros((4, tok), F32)], axis=0)
    meta[...] = lines.T
    emit_packs(cap, normed, queue, [([per * peers[k], per * peers[k] + 1], 0) for k in (2, 3)], far0, slots, sem)

    keep.wait()
    table[...] = jnp.zeros_like(table)
    table[0:1, :] = mine[0:1, :]
    for k, copy in enumerate(sends):
        copy.wait()
        table[k + 1:k + 2, :] = held[k, 0:1, :]


def route(hidden, idst, gain, w_router_t, group, cap):
    tok, width = hidden.shape
    experts = w_router_t.shape[0]
    one = jax.ShapeDtypeStruct((cap, width), BF16)
    return pl.pallas_call(
        functools.partial(route_kernel, group, experts // group, cap),
        out_shape=[jax.ShapeDtypeStruct((tok, width), BF16), jax.ShapeDtypeStruct((experts, tok), jnp.int32),
                   jax.ShapeDtypeStruct((tok, 8), F32), jax.ShapeDtypeStruct((8, 128), jnp.int32), one, one],
        in_specs=[HBM] + [VMEM] * 3,
        out_specs=[HBM] + [VMEM] * 3 + [HBM] * 2,
        scratch_shapes=[pltpu.VMEM((tok, width), BF16), pltpu.VMEM((tok, width), BF16), pltpu.SemaphoreType.DMA((5,)),
                        pltpu.VMEM((2, cap, width), BF16), pltpu.SemaphoreType.DMA((2,)),
                        pltpu.VMEM((8, 128), jnp.int32), pltpu.VMEM((2 * group - 1, 8, 128), jnp.int32),
                        pltpu.SemaphoreType.DMA((2 * group - 1,)), pltpu.SemaphoreType.DMA((2 * group - 1,))],
        cost_estimate=pl.CostEstimate(flops=10**10, bytes_accessed=2 * 10**7, transcendentals=0),
        compiler_params=pltpu.CompilerParams(collective_id=0, has_side_effects=True, vmem_limit_bytes=62 * MIB),
    )(hidden, idst, gain, w_router_t)


def pack_kernel(group, per, cap, jobs, n_out, normed, queue, *rest):
    outs, (slots, sem) = rest[:n_out], rest[n_out:]
    peers = peers_of(group)
    emit_packs(cap, normed, queue, [([per * peers[k] + i for i in which], lo) for k, which, lo in jobs], outs, slots, sem)


def pack(jobs, sizes, normed, queue, group, cap):
    _, width = normed.shape
    n = len(sizes)
    return pl.pallas_call(
        functools.partial(pack_kernel, group, queue.shape[0] // group, cap, jobs, n),
        out_shape=[jax.ShapeDtypeStruct((size, width), BF16) for size in sizes],
        in_specs=[VMEM] * 2,
        out_specs=[HBM] * n,
        scratch_shapes=[pltpu.VMEM((len(jobs), cap, width), BF16), pltpu.SemaphoreType.DMA((n,))],
        cost_estimate=pl.CostEstimate(flops=9 * 10**9, bytes_accessed=2 * 10**7, transcendentals=0),
        compiler_params=pltpu.CompilerParams(vmem_limit_bytes=62 * MIB),
    )(normed, queue)


def move_rows(src, at, dst, to, count):
    def one(c, _):
        dst[pl.ds(pl.multiple_of(to + c * BLK, BLK), BLK), :] = src[pl.ds(pl.multiple_of(at + c * BLK, BLK), BLK), :]
        return 0

    lax.fori_loop(0, count // BLK, one, 0)


def ffn_kernel(mode, local, per, dist, cap, sizes, n_in, n_out, table, *refs):
    ins, (wg, wu, wd), refs = refs[:n_in], refs[n_in:n_in + 3], refs[n_in + 3:]
    outs, (xs, acc, bg, bu, bd, wsem, sem, *more) = refs[:n_out], refs[n_out:]
    steps = wg.shape[2] // TF
    expert = per * lax.axis_index("ep") + local
    n0 = pl.multiple_of((table[dist, expert] + BLK - 1) // BLK * BLK, BLK)
    rows = n0 + table[dist + 1, expert]

    def copies(f, slot):
        cols = pl.ds(pl.multiple_of(f * TF, TF), TF)
        return (pltpu.make_async_copy(wg.at[local, :, cols], bg.at[slot], wsem.at[0, slot]),
                pltpu.make_async_copy(wu.at[local, :, cols], bu.at[slot], wsem.at[1, slot]),
                pltpu.make_async_copy(wd.at[local, cols, :], bd.at[slot], wsem.at[2, slot]))

    def fetch(f, slot):
        for c in copies(f, slot):
            c.start()

    def start(copies):
        for c in copies:
            c.start()

    def wait(copies):
        for c in copies:
            c.wait()

    if mode == "far1":
        packed, tails = more
        first = [table[dist + k, expert - 1] for k in range(2)]
        loads = []
        for k in range(2):
            at = 0
            for x in ins[k:6:2]:
                loads.append(pltpu.make_async_copy(x, packed.at[k, pl.ds(at, x.shape[0])], sem.at[len(loads)]))
                at += x.shape[0]
            loads.append(pltpu.make_async_copy(ins[6 + k], tails.at[k], sem.at[len(loads)]))
        start(loads)
        fetch(0, 0)
        acc[...] = jnp.zeros_like(acc)
        wait(loads)
        for k, to in enumerate((0, n0)):
            move_rows(packed.at[k], (first[k] + BLK - 1) // BLK * BLK, xs, to, cap)
    else:
        load = [pltpu.make_async_copy(x.at[pl.ds(0, cap)], xs.at[pl.ds(to, cap)], sem.at[k])
                for k, (x, to) in enumerate(zip(ins, (0, n0)))]
        load[0].start()
        fetch(0, 0)
        load[0].wait()
        load[1].start()
        acc[...] = jnp.zeros_like(acc)
        load[1].wait()

    def step(f, _):
        slot = lax.rem(f, NBUF)
        for c in copies(f, slot):
            c.wait()

        @pl.when(f == 0)
        def _():
            for k in range(1, NBUF - 1):
                fetch(k, k)

        @pl.when(f + NBUF - 1 < steps)
        def _():
            fetch(f + NBUF - 1, lax.rem(f + NBUF - 1, NBUF))

        def tile(m):
            x = xs[0:m, :]
            g = jnp.dot(x, bg[slot], preferred_element_type=F32)
            u = jnp.dot(x, bu[slot], preferred_element_type=F32)
            a = (jax.nn.silu(g) * u).astype(BF16)
            acc[0:m, :] += jnp.dot(a, bd[slot], preferred_element_type=F32)

        low = 0
        for m in sizes:
            @pl.when((rows > low) & (rows <= m))
            def _():
                tile(m)

            low = m
        return 0

    lax.fori_loop(0, steps, step, 0)
    xs[...] = acc[...].astype(BF16)
    stores = []
    for k, at in enumerate((0, n0)):
        source = xs
        if mode == "far1":
            source = packed.at[k]
            move_rows(xs, at, source, 0, cap)

            @pl.when(first[k] > cap - TAIL)
            def _():
                move_rows(tails.at[k], 0, source, (table[dist + k, expert] + BLK - 1) // BLK * BLK, TAIL)

            at = 0
        for out in outs[k::2]:
            stores.append(pltpu.make_async_copy(source.at[pl.ds(at, out.shape[0])], out, sem.at[len(stores)]))
            at += out.shape[0]
    start(stores)
    wait(stores)


def ffn(mode, table, xs, out_rows, wg, wu, wd, local, dist, cap):
    width, inner = wg.shape[1:]
    sizes = tuple(2 * cap - back for back in (192, 160, 128, 96, 64, 0))
    return pl.pallas_call(
        functools.partial(ffn_kernel, mode, local, wg.shape[0], dist, cap, sizes, len(xs), len(out_rows)),
        out_shape=[jax.ShapeDtypeStruct((rows, width), BF16) for rows in out_rows],
        in_specs=[SMEM] + [ANY] * (3 + len(xs)),
        out_specs=[HBM] * len(out_rows),
        scratch_shapes=[pltpu.VMEM((2 * cap, width), BF16), pltpu.VMEM((2 * cap, width), F32),
                        pltpu.VMEM((NBUF, width, TF), BF16), pltpu.VMEM((NBUF, width, TF), BF16),
                        pltpu.VMEM((NBUF, TF, width), BF16),
                        pltpu.SemaphoreType.DMA((3, NBUF)), pltpu.SemaphoreType.DMA((8,))]
        + ([pltpu.VMEM((2, 2 * cap, width), BF16), pltpu.VMEM((2, TAIL, width), BF16)] if mode == "far1" else []),
        cost_estimate=pl.CostEstimate(flops=6 * 540 * width * inner, bytes_accessed=6 * width * inner, transcendentals=0),
        compiler_params=pltpu.CompilerParams(vmem_limit_bytes=62 * MIB),
    )(table, *xs, wg, wu, wd)


def merge_kernel(group, per, cap, n_buf, table, meta, hid, *refs):
    bufs, (out, held, tgt, sem) = refs[:n_buf], refs[n_buf:]
    cut = 4 * cap
    first = pl.program_id(0) == 0
    spots = [0]
    for buf in bufs:
        spots.append(spots[-1] + buf.shape[0])

    def copy(j):
        return pltpu.make_async_copy(bufs[j], held.at[pl.ds(spots[j], bufs[j].shape[0])], sem.at[j])

    @pl.when(first)
    def _():
        for j in range(n_buf):
            copy(j).start()
        peers = peers_of(group)
        lane = lax.broadcasted_iota(jnp.int32, tgt.shape, 1)
        want = jnp.full(tgt.shape, -2, jnp.int32)
        runs = []
        for k in range(2):
            for i in range(2):
                runs.append(((2 * k + i) * cap, cap, (per * peers[k] + i) * cap))
        for k in range(2):
            e0 = per * peers[2 + k]
            at = cut + 2 * k * cap
            n1 = table[0, e0 + 1]
            runs.append((at, cap - TAIL, e0 * cap))
            runs.append((at + cap - TAIL, n1, (e0 + 1) * cap))
            runs.append((at + cap - TAIL + (n1 + BLK - 1) // BLK * BLK, jnp.maximum(table[0, e0] - (cap - TAIL), 0),
                         e0 * cap + cap - TAIL))
        for at, count, code in runs:
            want = jnp.where((lane >= at) & (lane < at + count), code + lane - at, want)
        tgt[...] = want.astype(F32)
        for j in range(4):
            copy(j).wait()

    def fetch(lo, hi):
        pick = jnp.concatenate([(meta[:, s:s + 1] == tgt[0:1, lo:hi]).astype(F32).astype(BF16) for s in range(2)], axis=0)
        return jnp.dot(pick, held[lo:hi, :], preferred_element_type=F32)

    rows = meta.shape[0]
    got = fetch(0, cut)
    near = meta[:, 2:3] * got[:rows] + meta[:, 3:4] * got[rows:]

    @pl.when(first)
    def _():
        for j in range(4, n_buf):
            copy(j).wait()

    got = fetch(cut, 2 * cut)
    far = meta[:, 2:3] * got[:rows] + meta[:, 3:4] * got[rows:]
    out[...] = (hid[...].astype(F32) + (near + far)).astype(out.dtype)


def merge(table, meta, hidden, bufs, group, per, cap):
    tok, width = hidden.shape
    deep = 8 * cap
    rows = 256
    tile = pl.BlockSpec((rows, width), lambda i: (i, 0))
    return pl.pallas_call(
        functools.partial(merge_kernel, group, per, cap, len(bufs)),
        out_shape=jax.ShapeDtypeStruct((tok, width), BF16),
        grid=(tok // rows,),
        in_specs=[SMEM, pl.BlockSpec((rows, 8), lambda i: (i, 0)), tile] + [ANY] * len(bufs),
        out_specs=tile,
        scratch_shapes=[pltpu.VMEM((deep, width), BF16), pltpu.VMEM((8, deep), F32),
                        pltpu.SemaphoreType.DMA((len(bufs),))],
        cost_estimate=pl.CostEstimate(flops=4 * tok * deep * width, bytes_accessed=2 * 10**7, transcendentals=0),
        compiler_params=pltpu.CompilerParams(vmem_limit_bytes=62 * MIB),
    )(table, meta, hidden, *bufs)


def solution(mesh):
    token_spec = P(("dp", "ep"), None)
    expert_spec = P("ep", None, None)

    def local_block(hidden, expert_ids, norm_gain, w_router, w_gate, w_up, w_down):
        tok, _ = hidden.shape
        experts = w_router.shape[1]
        per = w_gate.shape[0]
        group = experts // per
        cap = (5 * tok + 2 * experts - 1) // (2 * experts)

        def swap(x, k):
            return lax.ppermute(x, "ep", [(i, i ^ k) for i in range(group)])

        def after(x, *earlier):
            return lax.optimization_barrier((x, *earlier))[0]

        idst = expert_ids.T
        normed, queue, meta, table, *far0 = route(
            hidden, idst, norm_gain, w_router.T, group, cap)
        got0 = [swap(far0[0], 2), swap(far0[1], 3)]
        kept = table[:, :experts]
        even, odd = kept[:, 0::2], kept[:, 1::2]
        spill_out = jnp.any(up_to(even, BLK) + odd > 2 * cap - TAIL)
        spill_back = jnp.any(up_to(odd, BLK) + jnp.maximum(even - (cap - TAIL), 0) > cap)

        def swap_if(spill, xs):
            return lax.cond(spill, lambda a, b: (swap(a, 2), swap(b, 3)), lambda a, b: (a, b), *xs)

        own0, sib0, b2, c2, b3, c3 = pack(
            [(0, (0,), 0), (1, (0,), 0), (2, (0, 1), cap), (3, (0, 1), cap)],
            [cap, cap, cap - TAIL, TAIL, cap - TAIL, TAIL], normed, queue, group, cap)
        sib0 = swap(sib0, 1)
        got1 = [swap(b2, 2), swap(b3, 3)]

        def run(mode, i, k, xs, rows, *earlier):
            return ffn(mode, after(table, *earlier), xs, rows, w_gate, w_up, w_down, i, k, cap)

        o_own0, o_sib0 = run("near", 0, 0, [own0, sib0], [cap] * 2)
        o_far0 = run("far0", 0, 2, got0, [cap - TAIL] * 2 + [TAIL] * 2, o_own0)
        own1, sib1 = pack([(0, (1,), 0), (1, (1,), 0)], [cap] * 2, after(normed, o_far0[0]), queue, group, cap)
        sib1 = swap(sib1, 1)
        extra = swap_if(spill_out, after((c2, c3), *got1))
        back0 = [swap(after(o_far0[j], *got1), 2 + j) for j in range(2)]
        o_far1 = run("far1", 1, 2, [*got0, *got1, *extra, *o_far0[2:]], [cap] * 2 + [TAIL] * 2, own1)
        back1 = [swap(o_far1[0], 2), swap(o_far1[1], 3)]
        back2 = swap_if(spill_back, o_far1[2:])
        o_own1, o_sib1 = run("near", 1, 0, [own1, sib1], [cap] * 2, *back2)
        sib_back0 = swap(after(o_sib0, o_far1[0]), 1)
        sib_back1 = swap(o_sib1, 1)
        bufs = [o_own0, o_own1, sib_back0, sib_back1]
        for j in range(2):
            bufs += [back0[j], back1[j], back2[j]]
        return merge(table, meta, hidden, bufs, group, per, cap)

    return jax.shard_map(local_block, mesh=mesh,
                         in_specs=(token_spec, token_spec, P(None), P(None, None), expert_spec, expert_spec, expert_spec),
                         out_specs=token_spec, check_vma=False)
```

```python
import functools

import jax
import jax.numpy as jnp
from jax import lax
from jax.experimental import pallas as pl
from jax.experimental.pallas import tpu as pltpu
from jax.sharding import PartitionSpec as P


NORM_EPS = 1e-5
F32 = jnp.float32
BF16 = jnp.bfloat16
BLK = 16
TAIL = 48
NBUF = 3
TF = 512
ANY = pl.BlockSpec(memory_space=pl.ANY)
SMEM = pl.BlockSpec(memory_space=pltpu.SMEM)
VMEM = pl.BlockSpec(memory_space=pltpu.VMEM)
HBM = pl.BlockSpec(memory_space=pltpu.HBM)
MIB = 2**20


def up_to(n, m):
    return (n + m - 1) // m * m


def peers_of(group):
    me = lax.axis_index("ep")
    return [me, me + 1 - 2 * lax.rem(me, 2), lax.rem(me + 2, group), group - 1 - me]


def pack_rows(normed, queue, wanted, lo, count):
    rows = lo + lax.broadcasted_iota(jnp.int32, (count, queue.shape[1]), 0)
    hit, shift = None, None
    for expert in wanted:
        place = queue[pl.ds(expert, 1), :]
        kept = place >= 0
        at = place if shift is None else jnp.where(kept, place + shift, -1)
        here = rows == at
        hit = here if hit is None else hit | here
        held = jnp.sum(kept.astype(F32), axis=1, keepdims=True).astype(jnp.int32)
        shift = (held + (BLK - 1)) // BLK * BLK
    return jnp.dot(hit.astype(F32).astype(BF16), normed, preferred_element_type=F32).astype(BF16)


def emit_packs(cap, normed, queue, jobs, outs, slots, sem):
    copies = []
    outs = list(outs)
    for k, (wanted, lo) in enumerate(jobs):
        slots[k] = pack_rows(normed[...], queue, wanted, lo, cap)
        at = 0
        while at < cap:
            out = outs.pop(0)
            copies.append(pltpu.make_async_copy(slots.at[k, pl.ds(at, out.shape[0])], out, sem.at[len(copies)]))
            copies[-1].start()
            at += out.shape[0]
    for copy in copies:
        copy.wait()


def route_kernel(group, per, cap, hid_hbm, idst, gain, w_router_t, normed_hbm, queue, meta, table, *rest):
    far0, (hid, normed, row_sem, slots, sem, mine, held, send_sem, recv_sem) = rest[:2], rest[2:]
    tok = hid.shape[0]
    step = 256
    loads = [pltpu.make_async_copy(hid_hbm.at[pl.ds(i, step)], hid.at[pl.ds(i, step)], row_sem.at[i // step])
             for i in range(0, tok, step)]
    for copy in loads:
        copy.start()
    peers = peers_of(group)
    other = 1 - lax.axis_index("dp")
    mates = [{"ep": peer} for peer in peers[1:]] + [{"dp": other, "ep": peer} for peer in peers]
    barrier = pltpu.get_barrier_semaphore()
    for mate in mates:
        pl.semaphore_signal(barrier, inc=1, device_id=mate, device_id_type=pl.DeviceIdType.MESH)

    experts = w_router_t.shape[0]
    eye = lax.broadcasted_iota(jnp.int32, (experts, tok), 0)
    hit0 = (idst[0:1, :] == eye).astype(F32)
    hit1 = (idst[1:2, :] == eye).astype(F32)
    both = jnp.concatenate([hit0, hit1], axis=0).astype(BF16)
    total = lax.dot_general(jnp.ones((8, tok), BF16), (hit0 + hit1).astype(BF16), (((1,), (1,)), ((), ())),
                            preferred_element_type=F32)
    mine[...] = jnp.zeros_like(mine)
    mine[:, 0:experts] = jnp.minimum(total, float(cap)).astype(jnp.int32)

    for i in range(0, tok, step):
        loads[i // step].wait()
        x = hid[i:i + step, :].astype(F32)
        mean_sq = jnp.mean(x * x, axis=-1, keepdims=True)
        normed[i:i + step, :] = (x * lax.rsqrt(mean_sq + NORM_EPS) * gain[...].astype(F32).reshape(1, -1)).astype(BF16)

    keep = pltpu.make_async_copy(normed, normed_hbm, row_sem.at[tok // step])
    keep.start()
    pl.semaphore_wait(barrier, len(mates))
    sends = [pltpu.make_async_remote_copy(
        src_ref=mine, dst_ref=held.at[k], send_sem=send_sem.at[k], recv_sem=recv_sem.at[k],
        device_id=mate, device_id_type=pl.DeviceIdType.MESH) for k, mate in enumerate(mates)]
    for copy in sends:
        copy.start()

    logits = lax.dot_general(w_router_t[...], normed[...], (((1,), (1,)), ((), ())), preferred_element_type=F32)
    tot0 = jnp.sum(hit0, axis=1, keepdims=True)
    parts = []
    for i in range(0, tok, step):
        before = (lax.broadcasted_iota(jnp.int32, (tok, step), 0)
                  < i + lax.broadcasted_iota(jnp.int32, (tok, step), 1)).astype(F32).astype(BF16)
        parts.append(jnp.dot(both, before, preferred_element_type=F32))
    seen = jnp.concatenate(parts, axis=1)
    place = jnp.where(hit0 > 0, seen[:experts], jnp.where(hit1 > 0, seen[experts:] + tot0, -1.0))
    queue[...] = jnp.where(place < float(cap), place, -1.0).astype(jnp.int32)

    code = jnp.where(place < float(cap), eye.astype(F32) * float(cap) + place, -1.0)
    l0 = jnp.sum(hit0 * logits, axis=0, keepdims=True)
    l1 = jnp.sum(hit1 * logits, axis=0, keepdims=True)
    top = jnp.maximum(l0, l1)
    e0, e1 = jnp.exp(l0 - top), jnp.exp(l1 - top)
    lines = jnp.concatenate([jnp.sum(hit0 * code, axis=0, keepdims=True), jnp.sum(hit1 * code, axis=0, keepdims=True),
                             e0 / (e0 + e1), e1 / (e0 + e1), jnp.zeros((4, tok), F32)], axis=0)
    meta[...] = lines.T
    emit_packs(cap, normed, queue, [([per * peers[k], per * peers[k] + 1], 0) for k in (2, 3)], far0, slots, sem)

    keep.wait()
    table[...] = jnp.zeros_like(table)
    table[0:1, :] = mine[0:1, :]
    for k, copy in enumerate(sends):
        copy.wait()
        table[k + 1:k + 2, :] = held[k, 0:1, :]


def route(hidden, idst, gain, w_router_t, group, cap):
    tok, width = hidden.shape
    experts = w_router_t.shape[0]
    one = jax.ShapeDtypeStruct((cap, width), BF16)
    return pl.pallas_call(
        functools.partial(route_kernel, group, experts // group, cap),
        out_shape=[jax.ShapeDtypeStruct((tok, width), BF16), jax.ShapeDtypeStruct((experts, tok), jnp.int32),
                   jax.ShapeDtypeStruct((tok, 8), F32), jax.ShapeDtypeStruct((8, 128), jnp.int32), one, one],
        in_specs=[HBM] + [VMEM] * 3,
        out_specs=[HBM] + [VMEM] * 3 + [HBM] * 2,
        scratch_shapes=[pltpu.VMEM((tok, width), BF16), pltpu.VMEM((tok, width), BF16), pltpu.SemaphoreType.DMA((5,)),
                        pltpu.VMEM((2, cap, width), BF16), pltpu.SemaphoreType.DMA((2,)),
                        pltpu.VMEM((8, 128), jnp.int32), pltpu.VMEM((2 * group - 1, 8, 128), jnp.int32),
                        pltpu.SemaphoreType.DMA((2 * group - 1,)), pltpu.SemaphoreType.DMA((2 * group - 1,))],
        cost_estimate=pl.CostEstimate(flops=10**10, bytes_accessed=2 * 10**7, transcendentals=0),
        compiler_params=pltpu.CompilerParams(collective_id=0, has_side_effects=True, vmem_limit_bytes=62 * MIB),
    )(hidden, idst, gain, w_router_t)


def pack_kernel(group, per, cap, jobs, n_out, normed, queue, *rest):
    outs, (slots, sem) = rest[:n_out], rest[n_out:]
    peers = peers_of(group)
    emit_packs(cap, normed, queue, [([per * peers[k] + i for i in which], lo) for k, which, lo in jobs], outs, slots, sem)


def pack(jobs, sizes, normed, queue, group, cap):
    _, width = normed.shape
    n = len(sizes)
    return pl.pallas_call(
        functools.partial(pack_kernel, group, queue.shape[0] // group, cap, jobs, n),
        out_shape=[jax.ShapeDtypeStruct((size, width), BF16) for size in sizes],
        in_specs=[VMEM] * 2,
        out_specs=[HBM] * n,
        scratch_shapes=[pltpu.VMEM((len(jobs), cap, width), BF16), pltpu.SemaphoreType.DMA((n,))],
        cost_estimate=pl.CostEstimate(flops=9 * 10**9, bytes_accessed=2 * 10**7, transcendentals=0),
        compiler_params=pltpu.CompilerParams(vmem_limit_bytes=62 * MIB),
    )(normed, queue)


def move_rows(src, at, dst, to, count):
    def one(c, _):
        dst[pl.ds(pl.multiple_of(to + c * BLK, BLK), BLK), :] = src[pl.ds(pl.multiple_of(at + c * BLK, BLK), BLK), :]
        return 0

    lax.fori_loop(0, count // BLK, one, 0)


def ffn_kernel(mode, local, per, dist, cap, sizes, n_in, n_out, table, *refs):
    ins, (wg, wu, wd), refs = refs[:n_in], refs[n_in:n_in + 3], refs[n_in + 3:]
    outs, (xs, acc, bg, bu, bd, wsem, sem, *more) = refs[:n_out], refs[n_out:]
    steps = wg.shape[2] // TF
    expert = per * lax.axis_index("ep") + local
    n0 = pl.multiple_of((table[dist, expert] + BLK - 1) // BLK * BLK, BLK)
    rows = n0 + table[dist + 1, expert]

    def copies(f, slot):
        cols = pl.ds(pl.multiple_of(f * TF, TF), TF)
        return (pltpu.make_async_copy(wg.at[local, :, cols], bg.at[slot], wsem.at[0, slot]),
                pltpu.make_async_copy(wu.at[local, :, cols], bu.at[slot], wsem.at[1, slot]),
                pltpu.make_async_copy(wd.at[local, cols, :], bd.at[slot], wsem.at[2, slot]))

    def fetch(f, slot):
        for c in copies(f, slot):
            c.start()

    def start(copies):
        for c in copies:
            c.start()

    def wait(copies):
        for c in copies:
            c.wait()

    if mode == "far1":
        packed, tails = more
        first = [table[dist + k, expert - 1] for k in range(2)]
        loads = []
        for k in range(2):
            at = 0
            for x in ins[k:6:2]:
                loads.append(pltpu.make_async_copy(x, packed.at[k, pl.ds(at, x.shape[0])], sem.at[len(loads)]))
                at += x.shape[0]
            loads.append(pltpu.make_async_copy(ins[6 + k], tails.at[k], sem.at[len(loads)]))
        start(loads)
        fetch(0, 0)
        acc[...] = jnp.zeros_like(acc)
        wait(loads)
        for k, to in enumerate((0, n0)):
            move_rows(packed.at[k], (first[k] + BLK - 1) // BLK * BLK, xs, to, cap)
    else:
        load = [pltpu.make_async_copy(x.at[pl.ds(0, cap)], xs.at[pl.ds(to, cap)], sem.at[k])
                for k, (x, to) in enumerate(zip(ins, (0, n0)))]
        load[0].start()
        fetch(0, 0)
        load[0].wait()
        load[1].start()
        acc[...] = jnp.zeros_like(acc)
        load[1].wait()

    def step(f, _):
        slot = lax.rem(f, NBUF)
        for c in copies(f, slot):
            c.wait()

        @pl.when(f == 0)
        def _():
            for k in range(1, NBUF - 1):
                fetch(k, k)

        @pl.when(f + NBUF - 1 < steps)
        def _():
            fetch(f + NBUF - 1, lax.rem(f + NBUF - 1, NBUF))

        def tile(m):
            x = xs[0:m, :]
            g = jnp.dot(x, bg[slot], preferred_element_type=F32)
            u = jnp.dot(x, bu[slot], preferred_element_type=F32)
            a = (jax.nn.silu(g) * u).astype(BF16)
            acc[0:m, :] += jnp.dot(a, bd[slot], preferred_element_type=F32)

        low = 0
        for m in sizes:
            @pl.when((rows > low) & (rows <= m))
            def _():
                tile(m)

            low = m
        return 0

    lax.fori_loop(0, steps, step, 0)
    xs[...] = acc[...].astype(BF16)
    stores = []
    for k, at in enumerate((0, n0)):
        source = xs
        if mode == "far1":
            source = packed.at[k]
            move_rows(xs, at, source, 0, cap)

            @pl.when(first[k] > cap - TAIL)
            def _():
                move_rows(tails.at[k], 0, source, (table[dist + k, expert] + BLK - 1) // BLK * BLK, TAIL)

            at = 0
        for out in outs[k::2]:
            stores.append(pltpu.make_async_copy(source.at[pl.ds(at, out.shape[0])], out, sem.at[len(stores)]))
            at += out.shape[0]
    start(stores)
    wait(stores)


def ffn(mode, table, xs, out_rows, wg, wu, wd, local, dist, cap):
    width, inner = wg.shape[1:]
    sizes = tuple(2 * cap - back for back in (192, 160, 128, 96, 64, 0))
    return pl.pallas_call(
        functools.partial(ffn_kernel, mode, local, wg.shape[0], dist, cap, sizes, len(xs), len(out_rows)),
        out_shape=[jax.ShapeDtypeStruct((rows, width), BF16) for rows in out_rows],
        in_specs=[SMEM] + [ANY] * (3 + len(xs)),
        out_specs=[HBM] * len(out_rows),
        scratch_shapes=[pltpu.VMEM((2 * cap, width), BF16), pltpu.VMEM((2 * cap, width), F32),
                        pltpu.VMEM((NBUF, width, TF), BF16), pltpu.VMEM((NBUF, width, TF), BF16),
                        pltpu.VMEM((NBUF, TF, width), BF16),
                        pltpu.SemaphoreType.DMA((3, NBUF)), pltpu.SemaphoreType.DMA((8,))]
        + ([pltpu.VMEM((2, 2 * cap, width), BF16), pltpu.VMEM((2, TAIL, width), BF16)] if mode == "far1" else []),
        cost_estimate=pl.CostEstimate(flops=6 * 540 * width * inner, bytes_accessed=6 * width * inner, transcendentals=0),
        compiler_params=pltpu.CompilerParams(vmem_limit_bytes=62 * MIB),
    )(table, *xs, wg, wu, wd)


def merge_kernel(group, per, cap, n_buf, far, table, meta, *refs):
    base, refs = refs[:2 * far], refs[2 * far:]
    bufs, (out, held, tgt, sem) = refs[:n_buf], refs[n_buf:]
    spots = [0]
    for buf in bufs:
        spots.append(spots[-1] + buf.shape[0])

    @pl.when(pl.program_id(0) == 0)
    def _():
        copies = [pltpu.make_async_copy(buf, held.at[pl.ds(spots[j], buf.shape[0])], sem.at[j])
                  for j, buf in enumerate(bufs)]
        for copy in copies:
            copy.start()
        peers = peers_of(group)
        lane = lax.broadcasted_iota(jnp.int32, tgt.shape, 1)
        want = jnp.full(tgt.shape, -2, jnp.int32)
        runs = []
        for k in range(2):
            if far:
                e0 = per * peers[2 + k]
                at = 2 * k * cap
                n1 = table[0, e0 + 1]
                runs.append((at, cap - TAIL, e0 * cap))
                runs.append((at + cap - TAIL, n1, (e0 + 1) * cap))
                runs.append((at + cap - TAIL + (n1 + BLK - 1) // BLK * BLK,
                             jnp.maximum(table[0, e0] - (cap - TAIL), 0), e0 * cap + cap - TAIL))
            else:
                runs += [((2 * k + i) * cap, cap, (per * peers[k] + i) * cap) for i in range(2)]
        for at, count, code in runs:
            want = jnp.where((lane >= at) & (lane < at + count), code + lane - at, want)
        tgt[...] = want.astype(F32)
        for copy in copies:
            copy.wait()

    rows = meta.shape[0]
    pick = jnp.concatenate([(meta[:, s:s + 1] == tgt[0:1, :]).astype(F32).astype(BF16) for s in range(2)], axis=0)
    got = jnp.dot(pick, held[...], preferred_element_type=F32)
    total = meta[:, 2:3] * got[:rows] + meta[:, 3:4] * got[rows:]
    if far:
        total = base[1][...].astype(F32) + (base[0][...] + total)
    out[...] = total.astype(out.dtype)


def merge(table, meta, bufs, group, per, cap, base=()):
    tok, width = meta.shape[0], bufs[0].shape[1]
    deep = 4 * cap
    rows = 256
    tile = pl.BlockSpec((rows, width), lambda i: (i, 0))
    return pl.pallas_call(
        functools.partial(merge_kernel, group, per, cap, len(bufs), len(base) > 0),
        out_shape=jax.ShapeDtypeStruct((tok, width), BF16 if base else F32),
        grid=(tok // rows,),
        in_specs=[SMEM, pl.BlockSpec((rows, 8), lambda i: (i, 0))] + [tile] * len(base) + [ANY] * len(bufs),
        out_specs=tile,
        scratch_shapes=[pltpu.VMEM((deep, width), BF16), pltpu.VMEM((8, deep), F32),
                        pltpu.SemaphoreType.DMA((len(bufs),))],
        cost_estimate=pl.CostEstimate(flops=4 * tok * deep * width, bytes_accessed=2 * 10**7, transcendentals=0),
        compiler_params=pltpu.CompilerParams(vmem_limit_bytes=62 * MIB),
    )(table, meta, *base, *bufs)


def solution(mesh):
    token_spec = P(("dp", "ep"), None)
    expert_spec = P("ep", None, None)

    def local_block(hidden, expert_ids, norm_gain, w_router, w_gate, w_up, w_down):
        tok, _ = hidden.shape
        experts = w_router.shape[1]
        per = w_gate.shape[0]
        group = experts // per
        cap = (5 * tok + 2 * experts - 1) // (2 * experts)

        def swap(x, k):
            return lax.ppermute(x, "ep", [(i, i ^ k) for i in range(group)])

        def after(x, *earlier):
            return lax.optimization_barrier((x, *earlier))[0]

        idst = expert_ids.T
        normed, queue, meta, table, *far0 = route(
            hidden, idst, norm_gain, w_router.T, group, cap)
        got0 = [swap(far0[0], 2), swap(far0[1], 3)]
        kept = table[:, :experts]
        even, odd = kept[:, 0::2], kept[:, 1::2]
        spill_out = jnp.any(up_to(even, BLK) + odd > 2 * cap - TAIL)
        spill_back = jnp.any(up_to(odd, BLK) + jnp.maximum(even - (cap - TAIL), 0) > cap)

        def swap_if(spill, xs):
            return lax.cond(spill, lambda a, b: (swap(a, 2), swap(b, 3)), lambda a, b: (a, b), *xs)

        own0, sib0, b2, c2, b3, c3, own1, sib1 = pack(
            [(0, (0,), 0), (1, (0,), 0), (2, (0, 1), cap), (3, (0, 1), cap), (0, (1,), 0), (1, (1,), 0)],
            [cap, cap, cap - TAIL, TAIL, cap - TAIL, TAIL, cap, cap], normed, queue, group, cap)
        sib0, sib1 = swap(sib0, 1), swap(sib1, 1)
        got1 = [swap(b2, 2), swap(b3, 3)]

        def run(mode, i, k, xs, rows, *earlier):
            return ffn(mode, after(table, *earlier), xs, rows, w_gate, w_up, w_down, i, k, cap)

        o_own0, o_sib0 = run("near", 0, 0, [own0, sib0], [cap] * 2)
        o_far0 = run("far0", 0, 2, got0, [cap - TAIL] * 2 + [TAIL] * 2, o_own0)
        extra = swap_if(spill_out, after((c2, c3), *got1))
        back0 = [swap(after(o_far0[j], *got1), 2 + j) for j in range(2)]
        o_far1 = run("far1", 1, 2, [*got0, *got1, *extra, *o_far0[2:]], [cap] * 2 + [TAIL] * 2)
        back1 = [swap(o_far1[0], 2), swap(o_far1[1], 3)]
        back2 = swap_if(spill_back, o_far1[2:])
        o_own1, o_sib1 = run("near", 1, 0, [own1, sib1], [cap] * 2, *back2)
        sib_back0 = swap(after(o_sib0, o_far1[0]), 1)
        sib_back1 = swap(o_sib1, 1)
        near = merge(table, meta, [o_own0, o_own1, sib_back0, sib_back1], group, per, cap)
        bufs = []
        for j in range(2):
            bufs += [back0[j], back1[j], back2[j]]
        return merge(table, meta, bufs, group, per, cap, (near, hidden))

    return jax.shard_map(local_block, mesh=mesh,
                         in_specs=(token_spec, token_spec, P(None), P(None, None), expert_spec, expert_spec, expert_spec),
                         out_specs=token_spec, check_vma=False)
```

```python
import functools

import jax
import jax.numpy as jnp
from jax import lax
from jax.experimental import pallas as pl
from jax.experimental.pallas import tpu as pltpu
from jax.sharding import PartitionSpec as P


NORM_EPS = 1e-5
F32 = jnp.float32
BF16 = jnp.bfloat16
BLK = 16
TAIL = 48
NBUF = 3
TF = 512
ANY = pl.BlockSpec(memory_space=pl.ANY)
SMEM = pl.BlockSpec(memory_space=pltpu.SMEM)
VMEM = pl.BlockSpec(memory_space=pltpu.VMEM)
HBM = pl.BlockSpec(memory_space=pltpu.HBM)
MIB = 2**20


def up_to(n, m):
    return (n + m - 1) // m * m


def peers_of(group):
    me = lax.axis_index("ep")
    return [me, me + 1 - 2 * lax.rem(me, 2), lax.rem(me + 2, group), group - 1 - me]


def pack_rows(normed, queue, wanted, lo, count):
    rows = lo + lax.broadcasted_iota(jnp.int32, (count, queue.shape[1]), 0)
    hit, shift = None, None
    for expert in wanted:
        place = queue[pl.ds(expert, 1), :]
        kept = place >= 0
        at = place if shift is None else jnp.where(kept, place + shift, -1)
        here = rows == at
        hit = here if hit is None else hit | here
        held = jnp.sum(kept.astype(F32), axis=1, keepdims=True).astype(jnp.int32)
        shift = (held + (BLK - 1)) // BLK * BLK
    return jnp.dot(hit.astype(F32).astype(BF16), normed, preferred_element_type=F32).astype(BF16)


def emit_packs(cap, normed, queue, jobs, outs, slots, sem):
    copies = []
    outs = list(outs)
    for k, (wanted, lo) in enumerate(jobs):
        slots[k] = pack_rows(normed[...], queue, wanted, lo, cap)
        at = 0
        while at < cap:
            out = outs.pop(0)
            copies.append(pltpu.make_async_copy(slots.at[k, pl.ds(at, out.shape[0])], out, sem.at[len(copies)]))
            copies[-1].start()
            at += out.shape[0]
    for copy in copies:
        copy.wait()


def route_kernel(group, per, cap, hid_hbm, idst, gain, w_router_t, normed_hbm, queue, meta, table, *rest):
    far0, (hid, normed, row_sem, slots, sem, mine, held, send_sem, recv_sem) = rest[:2], rest[2:]
    tok = hid.shape[0]
    step = 256
    loads = [pltpu.make_async_copy(hid_hbm.at[pl.ds(i, step)], hid.at[pl.ds(i, step)], row_sem.at[i // step])
             for i in range(0, tok, step)]
    for copy in loads:
        copy.start()
    peers = peers_of(group)
    other = 1 - lax.axis_index("dp")
    mates = [{"ep": peer} for peer in peers[1:]] + [{"dp": other, "ep": peer} for peer in peers]
    barrier = pltpu.get_barrier_semaphore()
    for mate in mates:
        pl.semaphore_signal(barrier, inc=1, device_id=mate, device_id_type=pl.DeviceIdType.MESH)

    experts = w_router_t.shape[0]
    eye = lax.broadcasted_iota(jnp.int32, (experts, tok), 0)
    hit0 = (idst[0:1, :] == eye).astype(F32)
    hit1 = (idst[1:2, :] == eye).astype(F32)
    both = jnp.concatenate([hit0, hit1], axis=0).astype(BF16)
    total = lax.dot_general(jnp.ones((8, tok), BF16), (hit0 + hit1).astype(BF16), (((1,), (1,)), ((), ())),
                            preferred_element_type=F32)
    mine[...] = jnp.zeros_like(mine)
    mine[:, 0:experts] = jnp.minimum(total, float(cap)).astype(jnp.int32)

    for i in range(0, tok, step):
        loads[i // step].wait()
        x = hid[i:i + step, :].astype(F32)
        mean_sq = jnp.mean(x * x, axis=-1, keepdims=True)
        normed[i:i + step, :] = (x * lax.rsqrt(mean_sq + NORM_EPS) * gain[...].astype(F32).reshape(1, -1)).astype(BF16)

    keep = pltpu.make_async_copy(normed, normed_hbm, row_sem.at[tok // step])
    keep.start()
    pl.semaphore_wait(barrier, len(mates))
    sends = [pltpu.make_async_remote_copy(
        src_ref=mine, dst_ref=held.at[k], send_sem=send_sem.at[k], recv_sem=recv_sem.at[k],
        device_id=mate, device_id_type=pl.DeviceIdType.MESH) for k, mate in enumerate(mates)]
    for copy in sends:
        copy.start()

    logits = lax.dot_general(w_router_t[...], normed[...], (((1,), (1,)), ((), ())), preferred_element_type=F32)
    tot0 = jnp.sum(hit0, axis=1, keepdims=True)
    parts = []
    for i in range(0, tok, step):
        before = (lax.broadcasted_iota(jnp.int32, (tok, step), 0)
                  < i + lax.broadcasted_iota(jnp.int32, (tok, step), 1)).astype(F32).astype(BF16)
        parts.append(jnp.dot(both, before, preferred_element_type=F32))
    seen = jnp.concatenate(parts, axis=1)
    place = jnp.where(hit0 > 0, seen[:experts], jnp.where(hit1 > 0, seen[experts:] + tot0, -1.0))
    queue[...] = jnp.where(place < float(cap), place, -1.0).astype(jnp.int32)

    code = jnp.where(place < float(cap), eye.astype(F32) * float(cap) + place, -1.0)
    l0 = jnp.sum(hit0 * logits, axis=0, keepdims=True)
    l1 = jnp.sum(hit1 * logits, axis=0, keepdims=True)
    top = jnp.maximum(l0, l1)
    e0, e1 = jnp.exp(l0 - top), jnp.exp(l1 - top)
    lines = jnp.concatenate([jnp.sum(hit0 * code, axis=0, keepdims=True), jnp.sum(hit1 * code, axis=0, keepdims=True),
                             e0 / (e0 + e1), e1 / (e0 + e1), jnp.zeros((4, tok), F32)], axis=0)
    meta[...] = lines.T
    emit_packs(cap, normed, queue, [([per * peers[k], per * peers[k] + 1], 0) for k in (2, 3)], far0, slots, sem)

    keep.wait()
    table[...] = jnp.zeros_like(table)
    table[0:1, :] = mine[0:1, :]
    for k, copy in enumerate(sends):
        copy.wait()
        table[k + 1:k + 2, :] = held[k, 0:1, :]


def route(hidden, idst, gain, w_router_t, group, cap):
    tok, width = hidden.shape
    experts = w_router_t.shape[0]
    one = jax.ShapeDtypeStruct((cap, width), BF16)
    return pl.pallas_call(
        functools.partial(route_kernel, group, experts // group, cap),
        out_shape=[jax.ShapeDtypeStruct((tok, width), BF16), jax.ShapeDtypeStruct((experts, tok), jnp.int32),
                   jax.ShapeDtypeStruct((tok, 8), F32), jax.ShapeDtypeStruct((8, 128), jnp.int32), one, one],
        in_specs=[HBM] + [VMEM] * 3,
        out_specs=[HBM] + [VMEM] * 3 + [HBM] * 2,
        scratch_shapes=[pltpu.VMEM((tok, width), BF16), pltpu.VMEM((tok, width), BF16), pltpu.SemaphoreType.DMA((5,)),
                        pltpu.VMEM((2, cap, width), BF16), pltpu.SemaphoreType.DMA((2,)),
                        pltpu.VMEM((8, 128), jnp.int32), pltpu.VMEM((2 * group - 1, 8, 128), jnp.int32),
                        pltpu.SemaphoreType.DMA((2 * group - 1,)), pltpu.SemaphoreType.DMA((2 * group - 1,))],
        cost_estimate=pl.CostEstimate(flops=10**10, bytes_accessed=2 * 10**7, transcendentals=0),
        compiler_params=pltpu.CompilerParams(collective_id=0, has_side_effects=True, vmem_limit_bytes=62 * MIB),
    )(hidden, idst, gain, w_router_t)


def pack_kernel(group, per, cap, jobs, n_out, normed, queue, *rest):
    outs, (slots, sem) = rest[:n_out], rest[n_out:]
    peers = peers_of(group)
    emit_packs(cap, normed, queue, [([per * peers[k] + i for i in which], lo) for k, which, lo in jobs], outs, slots, sem)


def pack(jobs, sizes, normed, queue, group, cap):
    _, width = normed.shape
    n = len(sizes)
    return pl.pallas_call(
        functools.partial(pack_kernel, group, queue.shape[0] // group, cap, jobs, n),
        out_shape=[jax.ShapeDtypeStruct((size, width), BF16) for size in sizes],
        in_specs=[VMEM] * 2,
        out_specs=[HBM] * n,
        scratch_shapes=[pltpu.VMEM((len(jobs), cap, width), BF16), pltpu.SemaphoreType.DMA((n,))],
        cost_estimate=pl.CostEstimate(flops=9 * 10**9, bytes_accessed=2 * 10**7, transcendentals=0),
        compiler_params=pltpu.CompilerParams(vmem_limit_bytes=62 * MIB),
    )(normed, queue)


def move_rows(src, at, dst, to, count):
    def one(c, _):
        dst[pl.ds(pl.multiple_of(to + c * BLK, BLK), BLK), :] = src[pl.ds(pl.multiple_of(at + c * BLK, BLK), BLK), :]
        return 0

    lax.fori_loop(0, count // BLK, one, 0)


def ffn_kernel(mode, local, per, dist, cap, sizes, n_in, n_out, table, *refs):
    ins, (wg, wu, wd), refs = refs[:n_in], refs[n_in:n_in + 3], refs[n_in + 3:]
    outs, (xs, acc, bg, bu, bd, wsem, sem, *more) = refs[:n_out], refs[n_out:]
    steps = wg.shape[2] // TF
    expert = per * lax.axis_index("ep") + local
    n0 = pl.multiple_of((table[dist, expert] + BLK - 1) // BLK * BLK, BLK)
    rows = n0 + table[dist + 1, expert]

    def copies(f, slot):
        cols = pl.ds(pl.multiple_of(f * TF, TF), TF)
        return (pltpu.make_async_copy(wg.at[local, :, cols], bg.at[slot], wsem.at[0, slot]),
                pltpu.make_async_copy(wu.at[local, :, cols], bu.at[slot], wsem.at[1, slot]),
                pltpu.make_async_copy(wd.at[local, cols, :], bd.at[slot], wsem.at[2, slot]))

    def fetch(f, slot):
        for c in copies(f, slot):
            c.start()

    def start(copies):
        for c in copies:
            c.start()

    def wait(copies):
        for c in copies:
            c.wait()

    if mode == "far1":
        packed, tails = more
        first = [table[dist + k, expert - 1] for k in range(2)]
        loads = []
        for k in range(2):
            at = 0
            for x in ins[k:6:2]:
                loads.append(pltpu.make_async_copy(x, packed.at[k, pl.ds(at, x.shape[0])], sem.at[len(loads)]))
                at += x.shape[0]
            loads.append(pltpu.make_async_copy(ins[6 + k], tails.at[k], sem.at[len(loads)]))
        start(loads)
        fetch(0, 0)
        acc[...] = jnp.zeros_like(acc)
        wait(loads)
        for k, to in enumerate((0, n0)):
            move_rows(packed.at[k], (first[k] + BLK - 1) // BLK * BLK, xs, to, cap)
    else:
        load = [pltpu.make_async_copy(x.at[pl.ds(0, cap)], xs.at[pl.ds(to, cap)], sem.at[k])
                for k, (x, to) in enumerate(zip(ins, (0, n0)))]
        load[0].start()
        fetch(0, 0)
        load[0].wait()
        load[1].start()
        acc[...] = jnp.zeros_like(acc)
        load[1].wait()

    def step(f, _):
        slot = lax.rem(f, NBUF)
        for c in copies(f, slot):
            c.wait()

        @pl.when(f == 0)
        def _():
            for k in range(1, NBUF - 1):
                fetch(k, k)

        @pl.when(f + NBUF - 1 < steps)
        def _():
            fetch(f + NBUF - 1, lax.rem(f + NBUF - 1, NBUF))

        def tile(m):
            x = xs[0:m, :]
            g = jnp.dot(x, bg[slot], preferred_element_type=F32)
            u = jnp.dot(x, bu[slot], preferred_element_type=F32)
            a = (jax.nn.silu(g) * u).astype(BF16)
            acc[0:m, :] += jnp.dot(a, bd[slot], preferred_element_type=F32)

        low = 0
        for m in sizes:
            @pl.when((rows > low) & (rows <= m))
            def _():
                tile(m)

            low = m
        return 0

    lax.fori_loop(0, steps, step, 0)
    xs[...] = acc[...].astype(BF16)
    stores = []
    for k, at in enumerate((0, n0)):
        source = xs
        if mode == "far1":
            source = packed.at[k]
            move_rows(xs, at, source, 0, cap)

            @pl.when(first[k] > cap - TAIL)
            def _():
                move_rows(tails.at[k], 0, source, (table[dist + k, expert] + BLK - 1) // BLK * BLK, TAIL)

            at = 0
        for out in outs[k::2]:
            stores.append(pltpu.make_async_copy(source.at[pl.ds(at, out.shape[0])], out, sem.at[len(stores)]))
            at += out.shape[0]
    start(stores)
    wait(stores)


def ffn(mode, table, xs, out_rows, wg, wu, wd, local, dist, cap):
    width, inner = wg.shape[1:]
    sizes = tuple(2 * cap - back for back in (192, 160, 128, 96, 64, 0))
    return pl.pallas_call(
        functools.partial(ffn_kernel, mode, local, wg.shape[0], dist, cap, sizes, len(xs), len(out_rows)),
        out_shape=[jax.ShapeDtypeStruct((rows, width), BF16) for rows in out_rows],
        in_specs=[SMEM] + [ANY] * (3 + len(xs)),
        out_specs=[HBM] * len(out_rows),
        scratch_shapes=[pltpu.VMEM((2 * cap, width), BF16), pltpu.VMEM((2 * cap, width), F32),
                        pltpu.VMEM((NBUF, width, TF), BF16), pltpu.VMEM((NBUF, width, TF), BF16),
                        pltpu.VMEM((NBUF, TF, width), BF16),
                        pltpu.SemaphoreType.DMA((3, NBUF)), pltpu.SemaphoreType.DMA((8,))]
        + ([pltpu.VMEM((2, 2 * cap, width), BF16), pltpu.VMEM((2, TAIL, width), BF16)] if mode == "far1" else []),
        cost_estimate=pl.CostEstimate(flops=6 * 540 * width * inner, bytes_accessed=6 * width * inner, transcendentals=0),
        compiler_params=pltpu.CompilerParams(vmem_limit_bytes=62 * MIB),
    )(table, *xs, wg, wu, wd)


def merge_kernel(group, per, cap, n_buf, far, table, meta, *refs):
    base, refs = refs[:2 * far], refs[2 * far:]
    bufs, (out, held, tgt, sem) = refs[:n_buf], refs[n_buf:]
    spots = [0]
    for buf in bufs:
        spots.append(spots[-1] + buf.shape[0])

    @pl.when(pl.program_id(0) == 0)
    def _():
        copies = [pltpu.make_async_copy(buf, held.at[pl.ds(spots[j], buf.shape[0])], sem.at[j])
                  for j, buf in enumerate(bufs)]
        for copy in copies:
            copy.start()
        peers = peers_of(group)
        lane = lax.broadcasted_iota(jnp.int32, tgt.shape, 1)
        want = jnp.full(tgt.shape, -2, jnp.int32)
        runs = []
        for k in range(2):
            if far:
                e0 = per * peers[2 + k]
                at = 2 * k * cap
                n1 = table[0, e0 + 1]
                runs.append((at, cap - TAIL, e0 * cap))
                runs.append((at + cap - TAIL, n1, (e0 + 1) * cap))
                runs.append((at + cap - TAIL + (n1 + BLK - 1) // BLK * BLK,
                             jnp.maximum(table[0, e0] - (cap - TAIL), 0), e0 * cap + cap - TAIL))
            else:
                runs += [((2 * k + i) * cap, cap, (per * peers[k] + i) * cap) for i in range(2)]
        for at, count, code in runs:
            want = jnp.where((lane >= at) & (lane < at + count), code + lane - at, want)
        tgt[...] = want.astype(F32)
        for copy in copies:
            copy.wait()

    rows = meta.shape[0]
    pick = jnp.concatenate([(meta[:, s:s + 1] == tgt[0:1, :]).astype(F32).astype(BF16) for s in range(2)], axis=0)
    got = jnp.dot(pick, held[...], preferred_element_type=F32)
    total = meta[:, 2:3] * got[:rows] + meta[:, 3:4] * got[rows:]
    if far:
        total = base[1][...].astype(F32) + (base[0][...] + total)
    out[...] = total.astype(out.dtype)


def merge(table, meta, bufs, group, per, cap, base=()):
    tok, width = meta.shape[0], bufs[0].shape[1]
    deep = 4 * cap
    rows = 256
    tile = pl.BlockSpec((rows, width), lambda i: (i, 0))
    return pl.pallas_call(
        functools.partial(merge_kernel, group, per, cap, len(bufs), len(base) > 0),
        out_shape=jax.ShapeDtypeStruct((tok, width), BF16 if base else F32),
        grid=(tok // rows,),
        in_specs=[SMEM, pl.BlockSpec((rows, 8), lambda i: (i, 0))] + [tile] * len(base) + [ANY] * len(bufs),
        out_specs=tile,
        scratch_shapes=[pltpu.VMEM((deep, width), BF16), pltpu.VMEM((8, deep), F32),
                        pltpu.SemaphoreType.DMA((len(bufs),))],
        cost_estimate=pl.CostEstimate(flops=4 * tok * deep * width, bytes_accessed=2 * 10**7, transcendentals=0),
        compiler_params=pltpu.CompilerParams(vmem_limit_bytes=62 * MIB),
    )(table, meta, *base, *bufs)


def solution(mesh):
    token_spec = P(("dp", "ep"), None)
    expert_spec = P("ep", None, None)

    def local_block(hidden, expert_ids, norm_gain, w_router, w_gate, w_up, w_down):
        tok, _ = hidden.shape
        experts = w_router.shape[1]
        per = w_gate.shape[0]
        group = experts // per
        cap = (5 * tok + 2 * experts - 1) // (2 * experts)

        def swap(x, k):
            return lax.ppermute(x, "ep", [(i, i ^ k) for i in range(group)])

        def after(x, *earlier):
            return lax.optimization_barrier((x, *earlier))[0]

        idst = expert_ids.T
        normed, queue, meta, table, *far0 = route(
            hidden, idst, norm_gain, w_router.T, group, cap)
        got0 = [swap(far0[0], 2), swap(far0[1], 3)]
        kept = table[:, :experts]
        even, odd = kept[:, 0::2], kept[:, 1::2]
        spill_out = jnp.any(up_to(even, BLK) + odd > 2 * cap - TAIL)
        spill_back = jnp.any(up_to(odd, BLK) + jnp.maximum(even - (cap - TAIL), 0) > cap)

        def swap_if(spill, xs):
            return lax.cond(spill, lambda a, b: (swap(a, 2), swap(b, 3)), lambda a, b: (a, b), *xs)

        own0, sib0, b2, c2, b3, c3 = pack(
            [(0, (0,), 0), (1, (0,), 0), (2, (0, 1), cap), (3, (0, 1), cap)],
            [cap, cap, cap - TAIL, TAIL, cap - TAIL, TAIL], normed, queue, group, cap)
        own1, sib1 = pack([(0, (1,), 0), (1, (1,), 0)], [cap] * 2, after(normed, own0), queue, group, cap)
        sib0, sib1 = swap(sib0, 1), swap(sib1, 1)
        got1 = [swap(b2, 2), swap(b3, 3)]

        def run(mode, i, k, xs, rows, *earlier):
            return ffn(mode, after(table, *earlier), xs, rows, w_gate, w_up, w_down, i, k, cap)

        o_own0, o_sib0 = run("near", 0, 0, [own0, sib0], [cap] * 2, own1)
        o_far0 = run("far0", 0, 2, got0, [cap - TAIL] * 2 + [TAIL] * 2, o_own0)
        extra = swap_if(spill_out, after((c2, c3), *got1))
        back0 = [swap(after(o_far0[j], *got1), 2 + j) for j in range(2)]
        o_far1 = run("far1", 1, 2, [*got0, *got1, *extra, *o_far0[2:]], [cap] * 2 + [TAIL] * 2)
        back1 = [swap(o_far1[0], 2), swap(o_far1[1], 3)]
        back2 = swap_if(spill_back, o_far1[2:])
        o_own1, o_sib1 = run("near", 1, 0, [own1, sib1], [cap] * 2, *back2)
        sib_back0 = swap(after(o_sib0, o_far1[0]), 1)
        sib_back1 = swap(o_sib1, 1)
        near = merge(table, meta, [o_own0, o_own1, sib_back0, sib_back1], group, per, cap)
        bufs = []
        for j in range(2):
            bufs += [back0[j], back1[j], back2[j]]
        return merge(table, meta, bufs, group, per, cap, (near, hidden))

    return jax.shard_map(local_block, mesh=mesh,
                         in_specs=(token_spec, token_spec, P(None), P(None, None), expert_spec, expert_spec, expert_spec),
                         out_specs=token_spec, check_vma=False)
```
